32 devices in a mesh: scale: 2 (over y), lat: 16 (over z, x, core).
Axes of the slice: x: 2, y: 2, z: 4, core: 2. Of those that a mesh axis runs over, the one named last changes fastest.
Arguments:
- fine_state: float32 [16, 2, 1280, 1280], P(None, None, ('scale', 'lat')), may hold values from -6 to 6
- fine_noise: bfloat16 [16, 2, 1280, 1280], P(None, None, ('scale', 'lat')), may hold values from -6 to 6
- medium_state: float32 [16, 2, 640, 640], P(None, None, ('scale', 'lat')), may hold values from -6 to 6
- medium_noise: bfloat16 [16, 2, 640, 640], P(None, None, ('scale', 'lat')), may hold values from -6 to 6
- coarse_state: float32 [16, 2, 160, 160], P('lat'), may hold values from -6 to 6
- coarse_noise: bfloat16 [16, 2, 160, 160], P('lat'), may hold values from -6 to 6
- decay: float32 [3], replicated, may hold values from 0.5 to 0.95
- amplitude: float32 [3], replicated, may hold values from 0.3 to 1
- fine_basis: bfloat16 [1280, 32, 1280], P(('scale', 'lat')), may hold values from -0.0017089844 to 0.0017089844
- medium_basis: bfloat16 [640, 32, 640], P(('scale', 'lat')), may hold values from -0.0034179688 to 0.0034179688
- coarse_basis: bfloat16 [32, 160, 160], P(('scale', 'lat')), may hold values from -0.013671875 to 0.013671875
Outputs:
- fine_next: float32 [16, 2, 1280, 1280], P(None, None, ('scale', 'lat'))
- medium_next: float32 [16, 2, 640, 640], P(None, None, ('scale', 'lat'))
- coarse_next: float32 [16, 2, 160, 160], P('lat')
- pattern: float32 [16, 32, 2560], P(None, ('scale', 'lat'))
The draws below stay inside these ranges and needn't reach their ends.
All inputs are finite; a program needn't handle non-finite values.
Results may differ from the reference program's by a relative error of at most 0.005.
Values may be sent and summed in bfloat16 or wider, within the bound.
A program may use at most 128 MiB of HBM per device.

```python
import math
import jax
import jax.numpy as jnp
from jax import lax

MF = 1280
MM = 640
MC = 160
NLON = 2560
MEMBERS = 16
NROWS = 32


def shard_levels(own_key, dims, shards, smallest, largest):
    factor_of, own = 1.0, jax.random.fold_in(own_key, 6)
    for position, shards_of in shards:
        draws = jnp.exp(jax.random.uniform(jax.random.fold_in(own, position), (shards_of,), jnp.float32, smallest / len(shards), largest / len(shards)))
        factor_of = factor_of * jnp.repeat(draws, dims[position] // shards_of).reshape([-1 if axis == position else 1 for axis in range(len(dims))])
    return factor_of


def gaussian(own_key, dims, width, bound, pieces=(), held_as=jnp.bfloat16):
    factor_of = shard_levels(own_key, dims, pieces, -0.22, 0.18) if pieces else 1.0
    drawn = jax.random.normal(own_key, dims, jnp.float32) * width * factor_of
    return jnp.minimum(jnp.maximum(drawn, -bound), bound).astype(held_as)


def setup_inputs(seed: int = 0) -> dict:
    splits = jax.random.split(jax.random.key(seed), 12)
    fine_state = gaussian(splits[0], (MEMBERS, 2, MF, MF), 1.0, 6.0, ((2, 32),), jnp.float32)
    fine_noise = gaussian(splits[1], (MEMBERS, 2, MF, MF), 1.0, 6.0, ((2, 32),))
    medium_state = gaussian(splits[2], (MEMBERS, 2, MM, MM), 1.0, 6.0, ((2, 32),), jnp.float32)
    medium_noise = gaussian(splits[3], (MEMBERS, 2, MM, MM), 1.0, 6.0, ((2, 32),))
    coarse_state = gaussian(splits[4], (MEMBERS, 2, MC, MC), 1.0, 6.0, ((0, 16),), jnp.float32)
    coarse_noise = gaussian(splits[5], (MEMBERS, 2, MC, MC), 1.0, 6.0, ((0, 16),))
    decay = jnp.clip(jax.random.uniform(splits[6], (3,), jnp.float32, 0.5, 0.95), 0.5, 0.95)
    amplitude = jnp.clip(jax.random.uniform(splits[7], (3,), jnp.float32, 0.3, 1.0), 0.3, 1.0)
    fine_basis = gaussian(splits[8], (MF, NROWS, MF), (8 * MF * MF) ** -0.5, 0.0017089844, ((0, 32),))
    medium_basis = gaussian(splits[9], (MM, NROWS, MM), (8 * MM * MM) ** -0.5, 0.0034179688, ((0, 32),))
    coarse_basis = gaussian(splits[10], (NROWS, MC, MC), (8 * MC * MC) ** -0.5, 0.013671875, ((0, 32),))
    return {"fine_state": fine_state, "fine_noise": fine_noise, "medium_state": medium_state, "medium_noise": medium_noise, "coarse_state": coarse_state, "coarse_noise": coarse_noise, "decay": decay, "amplitude": amplitude, "fine_basis": fine_basis, "medium_basis": medium_basis, "coarse_basis": coarse_basis}


def advance(state, noise, decay_rate, amp_rate):
    slots = state.shape[3]
    mode_ids = jnp.arange(state.shape[2], dtype=jnp.int32)
    degree_ids = jnp.arange(slots, dtype=jnp.int32)
    inside = (mode_ids[:, None] + degree_ids[None, :]) < slots
    updated = decay_rate * state + amp_rate * noise.astype(jnp.float32)
    return jnp.where(inside, updated, jnp.zeros_like(updated))


def legendre_by_modes(half, basis):
    members, parts, modes, slots = half.shape
    nrow = basis.shape[1]
    blocks = modes // 32
    coef_blocks = jnp.moveaxis(half.reshape(members, parts, blocks, 32, slots), 2, 0)
    basis_blocks = basis.reshape(blocks, 32, nrow, slots)

    def one_block(pair):
        return jnp.einsum("ecmk,mrk->ecmr", pair[0].astype(jnp.float32), pair[1].astype(jnp.float32))

    result = lax.map(one_block, (coef_blocks, basis_blocks))
    return jnp.moveaxis(result, 0, 2).reshape(members, parts, modes, nrow)


def grid_table(modes):
    mode_ids = jnp.arange(modes, dtype=jnp.int32)
    lon_ids = jnp.arange(NLON, dtype=jnp.int32)
    angles = ((mode_ids[:, None] * lon_ids[None, :]) % NLON).astype(jnp.float32) * (2.0 * math.pi / NLON)
    weights = jnp.where(mode_ids == 0, 1.0, 2.0).astype(jnp.float32)[:, None]
    return jnp.stack([weights * jnp.cos(angles), -weights * jnp.sin(angles)]).astype(jnp.bfloat16)


def synthesis(fourier):
    table = grid_table(fourier.shape[2])
    return jnp.einsum("ecmr,cml->erl", fourier.astype(jnp.float32), table.astype(jnp.float32))


def reference(fine_state, fine_noise, medium_state, medium_noise, coarse_state, coarse_noise, decay, amplitude, fine_basis, medium_basis, coarse_basis):
    fine_next = advance(fine_state, fine_noise, decay[0], amplitude[0])
    medium_next = advance(medium_state, medium_noise, decay[1], amplitude[1])
    coarse_next = advance(coarse_state, coarse_noise, decay[2], amplitude[2])
    fine_fourier = legendre_by_modes(fine_next.astype(jnp.bfloat16), fine_basis).astype(jnp.bfloat16)
    medium_fourier = legendre_by_modes(medium_next.astype(jnp.bfloat16), medium_basis).astype(jnp.bfloat16)
    coarse_fourier = jnp.einsum("ecmk,rmk->ecmr", coarse_next.astype(jnp.bfloat16).astype(jnp.float32), coarse_basis.astype(jnp.float32)).astype(jnp.bfloat16)
    total = synthesis(fine_fourier) + synthesis(medium_fourier) + synthesis(coarse_fourier)
    pattern = jnp.tanh(total).astype(jnp.float32)
    return fine_next, medium_next, coarse_next, pattern
```

```python
import functools
import math

import jax
import jax.numpy as jnp
import numpy as np
from jax import lax
from jax.experimental import pallas as pl
from jax.experimental.pallas import tpu as pltpu
from jax.sharding import PartitionSpec as P

NLON = 2560
LANES = 128
FOLD = NLON // LANES


def advance(state, noise, decay_rate, amp_rate, offset):
    slots = state.shape[3]
    mode_ids = offset + jnp.arange(state.shape[2], dtype=jnp.int32)
    degree_ids = jnp.arange(slots, dtype=jnp.int32)
    inside = mode_ids[:, None] + degree_ids[None, :] < slots
    updated = decay_rate * state + amp_rate * noise.astype(jnp.float32)
    return jnp.where(inside, updated, jnp.zeros_like(updated))


def phase_rows(block, devices):
    return max((p * block % FOLD + block - 1) // FOLD + 1 for p in range(devices))


def phase_blocks(fourier, place, devices, modes=None):
    rows, parts, block, members = fourier.shape
    high = phase_rows(block, devices)
    if block % FOLD:
        start = (place * block % FOLD).astype(jnp.int32)
        room = jnp.zeros((rows, parts, high * FOLD, members), fourier.dtype)
        zero = jnp.zeros((), jnp.int32)
        fourier = lax.dynamic_update_slice(room, fourier, (zero, zero, start, zero))
    return fourier.reshape(rows, parts * high, FOLD * members)


def received_rows(blocks, devices, width):
    source = np.arange(devices, dtype=np.int32)
    cols, parts = [], []
    for block in blocks:
        for part in range(2):
            for j in range(phase_rows(block, devices)):
                cols.append(source * block // FOLD + j)
                parts.append(part)
    while len(cols) < width:
        cols.append(source * 0)
        parts.append(0)
    high = np.stack(cols, axis=1).reshape(-1, 1)
    part = np.tile(np.array(parts, np.int32), devices)[:, None]
    return np.concatenate([high, part], axis=1).astype(np.int32)


def table_kernel(rows_ref, table_ref):
    count = rows_ref.shape[0]
    high, part = rows_ref[:, 0:1], rows_ref[:, 1:2]
    lon = lax.broadcasted_iota(jnp.int32, (count, LANES), 1)
    turns = (high * lon + part * (LANES // 4)) % LANES
    angle = turns.astype(jnp.float32) * (2.0 * math.pi / LANES)
    re, im = 2.0 * jnp.cos(angle), 2.0 * jnp.sin(angle)
    first = jnp.where(high == 0, 0.5, 1.0).astype(jnp.float32)
    shape = (-(-FOLD // 8) * 8, LANES)
    low = lax.broadcasted_iota(jnp.int32, shape, 0) * lax.broadcasted_iota(jnp.int32, shape, 1)
    low = low.astype(jnp.float32) * (2.0 * math.pi / NLON)
    cos, sin = jnp.cos(low), jnp.sin(low)
    for q in range(FOLD):
        cl, sl = cos[q : q + 1], sin[q : q + 1]
        real, imag = re * cl - im * sl, im * cl + re * sl
        if q == 0:
            real, imag = real * first, imag * first
        table_ref[q, :, :LANES] = real.astype(jnp.bfloat16)
        table_ref[q, :, LANES:] = imag.astype(jnp.bfloat16)


def longitude_kernel(members, got_ref, table_ref, out_ref):
    own = got_ref.shape[1]
    for i in range(own):
        spread = got_ref[:, i].astype(jnp.float32)
        spread = spread.reshape(spread.shape[0] * spread.shape[1], spread.shape[2])
        lanes = -spread.shape[1] % LANES
        if lanes:
            spread = jnp.concatenate(
                [spread, jnp.zeros((spread.shape[0], lanes), jnp.float32)], axis=1
            )
        turned = spread.T.astype(jnp.bfloat16)
        totals = [None] * FOLD
        for q in range(FOLD):
            part = jnp.dot(
                turned[q * members : (q + 1) * members],
                table_ref[q],
                preferred_element_type=jnp.float32,
            )
            real, imag = part[:, :LANES], part[:, LANES:]
            for h in range(FOLD):
                turn = 2.0 * math.pi * (q * h % FOLD) / FOLD
                term = math.cos(turn) * real - math.sin(turn) * imag
                totals[h] = term if q == 0 else totals[h] + term
        for h in range(FOLD):
            out_ref[:, i, h * LANES : (h + 1) * LANES] = jnp.tanh(totals[h])


def coarse_kernel(
    part_modes, decay_ref, amp_ref, state_ref, noise_ref, basis_ref, next_ref, mixed_ref, fine_ref, medium_ref
):
    held, parts, modes, slots = state_ref.shape
    for scale, rate_ref in ((0, fine_ref), (1, medium_ref)):
        rate_ref[0:1] = jnp.full((1, rate_ref.shape[1]), decay_ref[scale], jnp.float32)
        rate_ref[1:2] = jnp.full((1, rate_ref.shape[1]), amp_ref[scale], jnp.float32)
    mode_ids = lax.broadcasted_iota(jnp.int32, (modes, slots), 0)
    degree_ids = lax.broadcasted_iota(jnp.int32, (modes, slots), 1)
    inside = mode_ids + degree_ids < slots
    planes = []
    for e in range(held):
        for c in range(parts):
            new = decay_ref[2] * state_ref[e, c] + amp_ref[2] * noise_ref[e, c].astype(jnp.float32)
            new = jnp.where(inside, new, 0.0)
            next_ref[e, c] = new
            planes.append(new)
    for r in range(basis_ref.shape[0]):
        planes.append(basis_ref[r].astype(jnp.float32))
    empty = jnp.zeros((part_modes, slots), jnp.float32)
    for d in range(mixed_ref.shape[0]):
        pieces = []
        for plane in planes:
            piece = plane[d * part_modes : min((d + 1) * part_modes, modes)]
            missing = part_modes - piece.shape[0]
            if missing == part_modes:
                piece = empty
            elif missing:
                piece = jnp.concatenate([piece, empty[:missing]], axis=0)
            pieces.append(piece)
        mixed_ref[d] = jnp.concatenate(pieces, axis=0).astype(jnp.bfloat16)


def general_body(
    fine_state,
    fine_noise,
    medium_state,
    medium_noise,
    coarse_state,
    coarse_noise,
    decay,
    amplitude,
    fine_basis,
    medium_basis,
    coarse_basis,
):
    devices = lax.axis_size("scale") * lax.axis_size("lat")
    lat = lax.axis_size("lat")
    held, _, modes, slots = coarse_state.shape
    own = coarse_basis.shape[0]
    part_modes = -(-modes // devices)
    vmem = pl.BlockSpec(memory_space=pltpu.VMEM)
    smem = pl.BlockSpec(memory_space=pltpu.SMEM)
    coarse_next, mixed, fine_rates, medium_rates = pl.pallas_call(
        functools.partial(coarse_kernel, part_modes),
        out_shape=(
            jax.ShapeDtypeStruct(coarse_state.shape, jnp.float32),
            jax.ShapeDtypeStruct((devices, (2 * held + own) * part_modes, slots), jnp.bfloat16),
            jax.ShapeDtypeStruct((2, fine_state.shape[3]), jnp.float32),
            jax.ShapeDtypeStruct((2, medium_state.shape[3]), jnp.float32),
        ),
        in_specs=[smem, smem, vmem, vmem, vmem],
        out_specs=(vmem,) * 4,
    )(decay, amplitude, coarse_state, coarse_noise, coarse_basis)
    mixed = lax.all_to_all(mixed, ("scale", "lat"), split_axis=0, concat_axis=0, tiled=True)
    mixed = mixed.reshape(devices, 2 * held + own, part_modes, slots)
    coarse_half = mixed[:lat, : 2 * held].reshape(lat * held, 2, part_modes, slots)
    coarse_rows = mixed[:, 2 * held :].reshape(devices * own, part_modes, slots)
    place = lax.axis_index(("scale", "lat"))
    fine_next = advance(fine_state, fine_noise, fine_rates[0], fine_rates[1], place * fine_state.shape[2])
    medium_next = advance(
        medium_state, medium_noise, medium_rates[0], medium_rates[1], place * medium_state.shape[2]
    )
    fourier = []
    for half, basis, form in (
        (fine_next.astype(jnp.bfloat16), fine_basis, "ecmk,mrk->rcme"),
        (medium_next.astype(jnp.bfloat16), medium_basis, "ecmk,mrk->rcme"),
        (coarse_half, coarse_rows, "ecmk,rmk->rcme"),
    ):
        fourier.append(
            jnp.einsum(form, half, basis, preferred_element_type=jnp.float32).astype(jnp.bfloat16)
        )
    members = coarse_half.shape[0]
    blocks = [x.shape[2] for x in fourier]
    both = jnp.concatenate([phase_blocks(x, place, devices) for x in fourier], axis=1)
    width = -(-both.shape[1] // 8) * 8
    both = jnp.pad(both, ((0, 0), (0, width - both.shape[1]), (0, 0)))
    received = received_rows(blocks, devices, width)
    table = pl.pallas_call(
        table_kernel,
        out_shape=jax.ShapeDtypeStruct((FOLD, devices * width, 2 * LANES), jnp.bfloat16),
        in_specs=[vmem],
        out_specs=vmem,
        cost_estimate=pl.CostEstimate(
            flops=30 * FOLD * devices * width * LANES,
            bytes_accessed=8 * FOLD * devices * width * LANES,
            transcendentals=4 * devices * width * LANES,
        ),
    )(jnp.asarray(received))
    got = lax.all_to_all(both, ("scale", "lat"), split_axis=0, concat_axis=0, tiled=True)
    got = got.reshape(devices, own, width, FOLD * members)
    pattern = pl.pallas_call(
        functools.partial(longitude_kernel, members),
        out_shape=jax.ShapeDtypeStruct((members, own, NLON), jnp.float32),
        in_specs=[vmem, vmem],
        out_specs=vmem,
    )(got, table)
    return (fine_next, medium_next, coarse_next, pattern)


MESH = pl.DeviceIdType.MESH
SUB = 8


class Sizes:
    def __init__(self, fine_state, medium_state, coarse_state, fine_basis, coarse_basis, scale, lat):
        self.scale, self.lat, self.n = scale, lat, scale * lat
        _, self.parts, self.fine, self.fine_slots = fine_state.shape
        self.members = fine_state.shape[0]
        self.pairs = self.members * self.parts
        self.medium, self.medium_slots = medium_state.shape[2:]
        self.coarse, self.coarse_slots = coarse_state.shape[2:]
        self.held, self.own, self.rows = coarse_state.shape[0], coarse_basis.shape[0], fine_basis.shape[1]
        self.groups = self.fine // SUB
        self.quad = LANES // self.pairs
        self.piece = self.coarse // lat
        self.wrap = NLON // max(self.quad, 1)

    def fits(self):
        if self.pairs * 4 != LANES or self.parts != 2 or self.held != 1 or self.own != 1:
            return False
        if self.rows != self.n or self.members != self.lat or self.members != 16:
            return False
        if self.fine % SUB or self.medium % 4 or self.fine != 2 * self.medium:
            return False
        if self.fine_slots % LANES or self.medium_slots % LANES or self.coarse % self.lat:
            return False
        if self.piece != 2 * (self.medium // 4) or 3 * self.piece > 32 or self.piece + 2 > 12:
            return False
        if not LANES < self.coarse_slots <= 2 * LANES or self.coarse_slots != self.coarse:
            return False
        high = self.fine // 4
        return SUB <= high and high - SUB + self.medium // 4 <= SUB and self.wrap % LANES == 0


def turns(count, columns, period, index):
    lon = lax.broadcasted_iota(jnp.int32, (count, columns), 1)
    angle = ((index * lon) % period).astype(jnp.float32) * (2.0 * math.pi / period)
    return jnp.cos(angle), jnp.sin(angle)


def spread_kernel(
    z,
    decay,
    amp,
    fine_state,
    fine_noise,
    fine_basis,
    medium_state,
    medium_noise,
    medium_basis,
    coarse_state,
    coarse_noise,
    coarse_basis,
    fine_next,
    medium_next,
    coarse_next,
    got,
    got_coarse,
    table,
    noise_f,
    basis_f,
    half,
    picked,
    noise_m,
    basis_m,
    half_m,
    rows_f,
    send,
    noise_c,
    basis_c,
    first,
    first_far,
    landed,
    landed_far,
    landed_f,
    left_c,
    right_c,
    rows_c,
    second,
    wave_cos,
    wave_sin,
    load_f,
    load_m,
    load_c,
    sent,
    came,
    sent_one,
    came_one,
    sent_far,
    came_far,
    sent_two,
    came_two,
):
    n, lat = z.n, z.lat
    s, a = lax.axis_index("scale"), lax.axis_index("lat")
    me = s * lat + a
    f32, bf16 = jnp.float32, jnp.bfloat16
    mid_tiles = z.medium_slots // LANES
    fine_quads, medium_quads = z.fine // 4, z.medium // 4
    far = -(-(z.coarse_slots - LANES) // z.piece)

    def place(p):
        return {"scale": p // lat, "lat": p % lat}

    barrier = pltpu.get_barrier_semaphore()

    def greet(i, _):
        pl.semaphore_signal(barrier, inc=1, device_id=place((me + i) % n), device_id_type=MESH)
        return 0

    lax.fori_loop(1, n, greet, 0)

    def coarse_loads():
        return (
            pltpu.make_async_copy(coarse_state.at[0], coarse_next, load_c.at[0]),
            pltpu.make_async_copy(coarse_noise.at[0], noise_c, load_c.at[1]),
            pltpu.make_async_copy(coarse_basis.at[0], basis_c, load_c.at[2]),
        )

    def fine_loads(g):
        rows = pl.ds(pl.multiple_of(g * SUB, SUB), SUB)
        return (
            pltpu.make_async_copy(fine_state.at[:, rows, :], fine_next.at[:, rows, :], load_f.at[0, g]),
            pltpu.make_async_copy(fine_noise.at[:, rows, :], noise_f.at[g], load_f.at[1, g]),
            pltpu.make_async_copy(fine_basis.at[rows], basis_f.at[rows], load_f.at[2, g]),
        )

    def medium_loads():
        copies = [pltpu.make_async_copy(medium_basis, basis_m, load_m.at[2 * mid_tiles])]
        for t in range(mid_tiles):
            cols = pl.ds(t * LANES, LANES)
            copies.append(
                pltpu.make_async_copy(medium_state.at[:, :, :, cols], medium_next.at[t], load_m.at[2 * t])
            )
            copies.append(
                pltpu.make_async_copy(medium_noise.at[:, :, :, cols], noise_m.at[t], load_m.at[2 * t + 1])
            )
        return copies

    for copy in coarse_loads():
        copy.start()
    for g in range(z.groups - 1):
        for copy in fine_loads(g):
            copy.start()
    for copy in medium_loads():
        copy.start()
    for copy in fine_loads(z.groups - 1):
        copy.start()

    for copy in coarse_loads():
        copy.wait()
    mode = lax.broadcasted_iota(jnp.int32, (z.coarse, z.coarse_slots), 0)
    degree = lax.broadcasted_iota(jnp.int32, (z.coarse, z.coarse_slots), 1)
    inside = mode + degree < z.coarse_slots
    planes = []
    for c in range(2):
        new = decay[2] * coarse_next[c] + amp[2] * noise_c[c].astype(f32)
        new = jnp.where(inside, new, 0.0)
        coarse_next[c] = new
        planes.append(new)
    planes.append(basis_c[...].astype(f32))
    fill = jnp.zeros((32 - 3 * z.piece, z.coarse_slots), f32)
    for p in range(lat):
        block = [plane[p * z.piece : (p + 1) * z.piece] for plane in planes]
        block = jnp.concatenate(block + [fill], axis=0).astype(bf16)
        first[p] = block[:, :LANES]
        if p < far:
            rest = block[:, LANES:].astype(f32)
            rest = jnp.concatenate([rest, jnp.zeros((32, 2 * LANES - z.coarse_slots), f32)], axis=1)
            first_far[p] = rest.astype(bf16)

    def first_copy(p):
        return pltpu.make_async_remote_copy(
            first.at[p], landed.at[a], sent_one.at[p], came_one.at[a],
            device_id={"scale": s, "lat": p}, device_id_type=MESH,
        )

    def far_copy(p):
        return pltpu.make_async_remote_copy(
            first_far.at[p], landed_far.at[a], sent_far.at[p], came_far.at[a],
            device_id={"scale": s, "lat": p}, device_id_type=MESH,
        )

    def second_copy(p):
        return pltpu.make_async_remote_copy(
            second.at[p], got_coarse.at[a], sent_two.at[p], came_two.at[a],
            device_id={"scale": s, "lat": p}, device_id_type=MESH,
        )

    def row_copy(t, p):
        return pltpu.make_async_remote_copy(
            send.at[t, p], got.at[t, me], sent.at[t, p], came.at[t, me],
            device_id=place(p), device_id_type=MESH,
        )

    lane = lax.broadcasted_iota(jnp.int32, (z.rows, 2 * LANES), 1) % SUB
    shift = lax.broadcasted_iota(jnp.int32, (SUB, z.fine_slots), 0)
    slack = z.fine_slots - me * z.fine - shift - lax.broadcasted_iota(jnp.int32, (SUB, z.fine_slots), 1)

    def fine_group(g, _):
        for copy in fine_loads(g):
            copy.wait()
        rows = pl.ds(pl.multiple_of(g * SUB, SUB), SUB)
        keep = slack > g * SUB

        def pair(i, _):
            new = decay[0] * fine_next[pl.ds(2 * i, 2), rows, :] + amp[0] * noise_f[g, pl.ds(2 * i, 2)].astype(f32)
            new = jnp.where(keep[None], new, 0.0)
            fine_next[pl.ds(2 * i, 2), rows, :] = new
            at = pl.ds(pl.multiple_of(2 * SUB * i, 2 * SUB), 2 * SUB)
            half[at, :] = new.reshape(2 * SUB, z.fine_slots).astype(bf16)
            return 0

        lax.fori_loop(0, z.pairs // 2, pair, 0)
        basis = basis_f[rows].reshape(SUB * z.rows, z.fine_slots)
        all_pairs = lax.dot_general(basis, half[...], (((1,), (1,)), ((), ())), preferred_element_type=f32)
        total = all_pairs[: z.rows]
        for q in range(1, SUB):
            total = jnp.where(lane == q, all_pairs[q * z.rows : (q + 1) * z.rows], total)
        picked[pl.ds(pl.multiple_of(g * z.rows, z.rows), z.rows), :] = total.astype(bf16)
        return 0

    target = lax.broadcasted_iota(jnp.int32, (2 * LANES, 2 * LANES), 1)
    wanted = (target % z.members) * (2 * SUB) + (target // z.members % 2) * SUB
    wanted = wanted + target // LANES * 4 + target // z.pairs % 4
    order = (lax.broadcasted_iota(jnp.int32, (2 * LANES, 2 * LANES), 0) == wanted).astype(f32).astype(bf16)
    stride = 3 * SUB

    def put_fine(g0, g1):
        moved = jnp.dot(picked[g0 * z.rows : g1 * z.rows, :], order, preferred_element_type=f32)
        for g in range(g0, g1):
            for q in range(2):
                rows_f[pl.ds(2 * g + q, z.rows, stride=stride), :] = moved[
                    (g - g0) * z.rows : (g - g0 + 1) * z.rows, q * LANES : (q + 1) * LANES
                ]

    line = lax.broadcasted_iota(jnp.int32, (SUB, LANES), 0)
    column = lax.broadcasted_iota(jnp.int32, (SUB, LANES), 1)

    def weight(row, index):
        at_zero = (line == row) & (column < z.pairs) & (index == 0)
        return jnp.where(at_zero, 0.5, 1.0).astype(f32)

    def ship(t):
        scale_row = weight(0 if t == 0 else fine_quads - SUB, me)

        def cast(r, _):
            at = pl.ds(pl.multiple_of(r * stride + t * SUB, SUB), SUB)
            send[t, r] = (rows_f[at, :].astype(bf16).astype(f32) * scale_row).astype(bf16)
            return 0

        lax.fori_loop(0, z.rows, cast, 0)

        def go(i, _):
            row_copy(t, (me + i) % n).start()
            return 0

        lax.fori_loop(1, n, go, 0)
        got[t, me] = send[t, me]

    lax.fori_loop(0, 2, fine_group, 0)
    pl.semaphore_wait(barrier, n - 1)

    def go_first(i, _):
        p = (a + i) % lat
        first_copy(p).start()

        @pl.when(p < far)
        def _():
            far_copy(p).start()

        return 0

    lax.fori_loop(1, lat, go_first, 0)
    landed[a] = first[a]

    @pl.when(a < far)
    def _():
        landed_far[a] = first_far[a]

    lax.fori_loop(2, z.groups - 1, fine_group, 0)
    put_fine(0, z.groups - 1)
    ship(0)

    for copy in medium_loads():
        copy.wait()
    flat_next = medium_next.reshape(mid_tiles * z.pairs * z.medium, LANES)
    flat_noise = noise_m.reshape(mid_tiles * z.pairs * z.medium, LANES)
    span = 2 * z.medium
    room = z.medium_slots - me * z.medium - lax.broadcasted_iota(jnp.int32, (span, LANES), 0) // 2
    room = room - lax.broadcasted_iota(jnp.int32, (span, LANES), 1)

    def medium_member(e, _):
        for t in range(mid_tiles):
            at = pl.ds(pl.multiple_of((t * z.members + e) * span, SUB), span)
            new = decay[1] * flat_next[at, :] + amp[1] * flat_noise[at, :].astype(f32)
            flat_next[at, :] = jnp.where(room > t * LANES, new, 0.0)
        return 0

    lax.fori_loop(0, z.members, medium_member, 0)

    def medium_mode(m, _):
        for c in range(2):
            at = pl.ds(pl.multiple_of(m * z.pairs + c * z.members, z.members), z.members)
            for t in range(mid_tiles):
                new = flat_next[pl.ds(t * z.members * span + 2 * m + c, z.members, stride=span), :]
                half_m[at, t * LANES : (t + 1) * LANES] = new.astype(bf16)
        return 0

    lax.fori_loop(0, z.medium, medium_mode, 0)
    lane4 = lax.broadcasted_iota(jnp.int32, (z.rows, LANES), 1) // z.pairs
    for q in range(medium_quads):
        basis = basis_m[4 * q : 4 * q + 4].reshape(4 * z.rows, z.medium_slots)
        all_pairs = lax.dot_general(
            basis, half_m[q * LANES : (q + 1) * LANES, :], (((1,), (1,)), ((), ())), preferred_element_type=f32
        )
        total = all_pairs[: z.rows]
        for b in range(1, 4):
            total = jnp.where(lane4 == b, all_pairs[b * z.rows : (b + 1) * z.rows], total)
        rows_f[pl.ds(fine_quads + q, z.rows, stride=stride), :] = total
    for spare in range(fine_quads + medium_quads, 2 * SUB):
        rows_f[pl.ds(spare, z.rows, stride=stride), :] = jnp.zeros((z.rows, LANES), f32)

    lax.fori_loop(z.groups - 1, z.groups, fine_group, 0)
    put_fine(z.groups - 1, z.groups)
    ship(1)

    def came_first(i, _):
        p = (a + i) % lat
        pltpu.make_async_remote_copy(
            first.at[p], landed.at[p], sent_one.at[p], came_one.at[p],
            device_id={"scale": s, "lat": p}, device_id_type=MESH,
        ).wait_recv()
        return 0

    lax.fori_loop(1, lat, came_first, 0)
    offset = (a * z.piece) % 4
    left_c[...] = jnp.zeros_like(left_c)
    right_c[...] = jnp.zeros_like(right_c)
    jump = 5 * SUB

    def lay(source, cols):
        def spread(p, _):
            landed_f[pl.ds(pl.multiple_of(p * jump, SUB), 32), :] = source[p].astype(f32)
            return 0

        lax.fori_loop(0, lat, spread, 0)
        for i in range(z.piece):
            for c in range(2):
                at = pl.ds(pl.multiple_of((i + offset) * z.pairs + c * z.members, z.members), z.members)
                values = landed_f[pl.ds(c * z.piece + i, lat, stride=jump), :]
                right_c[at, cols] = values.astype(bf16)
            at = pl.ds(pl.multiple_of((i + offset) * lat, lat), lat)
            left_c[at, cols] = landed_f[pl.ds(2 * z.piece + i, lat, stride=jump), :].astype(bf16)

    lay(landed, slice(0, LANES))

    @pl.when(a < far)
    def _():
        def came_rest(i, _):
            p = (a + i) % lat
            pltpu.make_async_remote_copy(
                first_far.at[0], landed_far.at[p], sent_far.at[0], came_far.at[p],
                device_id={"scale": s, "lat": p}, device_id_type=MESH,
            ).wait_recv()
            return 0

        lax.fori_loop(1, lat, came_rest, 0)
        lay(landed_far, slice(LANES, 2 * LANES))

    all_pairs = lax.dot_general(
        left_c[...], right_c[...], (((1,), (1,)), ((), ())), preferred_element_type=f32
    )
    slot = lax.broadcasted_iota(jnp.int32, (lat, 12 * z.pairs), 1) // z.pairs
    total = all_pairs[:lat]
    for b in range(1, 12):
        total = jnp.where(slot == b, all_pairs[b * lat : (b + 1) * lat], total)
    rows_c[...] = jnp.zeros_like(rows_c)
    for j in range(3):
        rows_c[pl.ds(j, lat, stride=SUB), :] = total[:, j * LANES : (j + 1) * LANES]
    scale_row = weight(0, a)
    for p in range(lat):
        second[p] = (rows_c[p * SUB : (p + 1) * SUB, :].astype(bf16).astype(f32) * scale_row).astype(bf16)

    def go_second(i, _):
        second_copy((a + i) % lat).start()
        return 0

    lax.fori_loop(1, lat, go_second, 0)
    got_coarse[a] = second[a]

    count = 2 * n
    step = medium_quads * lax.broadcasted_iota(jnp.int32, (count, z.wrap), 0)
    wave_cos[...], wave_sin[...] = turns(count, z.wrap, z.wrap, step)
    line = lax.broadcasted_iota(jnp.int32, (SUB, z.wrap), 0)
    cut = fine_quads - SUB

    def twice(index):
        cos, sin = turns(SUB, z.wrap, z.wrap, index)
        return 2.0 * cos, 2.0 * sin

    def turned(base, cos, sin):
        return base[0] * cos - base[1] * sin, base[0] * sin + base[1] * cos

    def keep_rows(at, upper, lower):
        for part in range(2):
            both = jnp.concatenate([upper[part], lower[part]], axis=0).astype(bf16)
            for t in range(z.wrap // LANES):
                lo = (2 * t + part) * LANES
                table[at, lo : lo + LANES] = both[:, t * LANES : (t + 1) * LANES]

    base = twice(line)
    base_mixed = twice(jnp.where(line < cut, SUB + line, line - cut))
    base_odd = twice(medium_quads // 2 + line)

    def wave(u):
        return wave_cos[pl.ds(u, 1), :], wave_sin[pl.ds(u, 1), :]

    def fill_rows(i, _):
        pair0, pair1 = [], []
        for k in range(2):
            p = 2 * i + k
            cos, sin = wave(2 * p)
            pair0.append(turned(base, cos, sin))
            low_cos, low_sin = wave(p)
            cos = jnp.where(line < cut, cos, low_cos)
            sin = jnp.where(line < cut, sin, low_sin)
            pair1.append(turned(base_mixed, cos, sin))
        at = pl.multiple_of(2 * SUB * i, 2 * SUB)
        keep_rows(pl.ds(at, 2 * SUB), *pair0)
        keep_rows(pl.ds(at + n * SUB, 2 * SUB), *pair1)
        return 0

    lax.fori_loop(0, n // 2, fill_rows, 0)

    def fill_coarse(i, _):
        cos, sin = wave(i)
        at = pl.multiple_of(2 * SUB * (i + n), 2 * SUB)
        keep_rows(pl.ds(at, 2 * SUB), turned(base, cos, sin), turned(base_odd, cos, sin))
        return 0

    lax.fori_loop(0, lat // 2, fill_coarse, 0)

    def came_rows(i, _):
        p = (me + i) % n
        for t in range(2):
            pltpu.make_async_remote_copy(
                send.at[t, p], got.at[t, p], sent.at[t, p], came.at[t, p],
                device_id=place(p), device_id_type=MESH,
            ).wait()
        return 0

    lax.fori_loop(1, n, came_rows, 0)

    def came_second(i, _):
        p = (a + i) % lat
        pltpu.make_async_remote_copy(
            second.at[p], got_coarse.at[p], sent_two.at[p], came_two.at[p],
            device_id={"scale": s, "lat": p}, device_id_type=MESH,
        ).wait()
        first_copy(p).wait_send()

        @pl.when(p < far)
        def _():
            far_copy(p).wait_send()

        return 0

    lax.fori_loop(1, lat, came_second, 0)


def grid_kernel(
    z, fine_in, medium_in, coarse_in, got, got_coarse, table, fine_out, medium_out, coarse_out, out, turned, sems
):
    copies = [
        pltpu.make_async_copy(fine_in, fine_out, sems.at[0]),
        pltpu.make_async_copy(coarse_in, coarse_out.at[0], sems.at[1]),
    ]
    for t in range(medium_in.shape[0]):
        cols = pl.ds(t * LANES, LANES)
        copies.append(pltpu.make_async_copy(medium_in.at[t], medium_out.at[:, :, :, cols], sems.at[2 + t]))
    for copy in copies:
        copy.start()
    many = 2 * z.n * SUB
    turned[:, :many] = got[...].reshape(many, LANES).astype(jnp.float32).T.astype(jnp.bfloat16)
    few = got_coarse[...].reshape(z.lat * SUB, LANES).astype(jnp.float32)
    turned[:, many:] = few.T.astype(jnp.bfloat16)
    e, tiles = z.members, z.wrap // LANES
    for t in range(tiles):
        both = jnp.dot(turned[...], table[:, 2 * t * LANES : 2 * (t + 1) * LANES], preferred_element_type=jnp.float32)
        waves = []
        for b in range(4):
            at = 2 * b * e
            cos_r, sin_r = both[at : at + e, :LANES], both[at : at + e, LANES:]
            cos_i, sin_i = both[at + e : at + 2 * e, :LANES], both[at + e : at + 2 * e, LANES:]
            re, im = cos_r - sin_i, sin_r + cos_i
            if b:
                angle = (lax.broadcasted_iota(jnp.int32, (1, LANES), 1) + t * LANES).astype(jnp.float32)
                angle = angle * (2.0 * math.pi * b / NLON)
                cos, sin = jnp.cos(angle), jnp.sin(angle)
                re, im = re * cos - im * sin, re * sin + im * cos
            waves.append((re, im))
        for h in range(4):
            total = None
            for b in range(4):
                re, im = waves[b]
                term = (re, -im, -re, im)[b * h % 4]
                total = term if total is None else total + term
            out[pl.ds(h * tiles + t, e, stride=4 * tiles), :] = jnp.tanh(total)
    for copy in copies:
        copy.wait()


def fast_body(
    z,
    fine_state,
    fine_noise,
    medium_state,
    medium_noise,
    coarse_state,
    coarse_noise,
    decay,
    amplitude,
    fine_basis,
    medium_basis,
    coarse_basis,
):
    f32, bf16, dma = jnp.float32, jnp.bfloat16, pltpu.SemaphoreType.DMA
    e, n, lat, rows = z.members, z.n, z.lat, z.rows
    tiles = z.medium_slots // LANES
    far = -(-(z.coarse_slots - LANES) // z.piece)
    table_rows = (2 * n + lat) * SUB
    operands = (
        fine_state.reshape(z.pairs, z.fine, z.fine_slots),
        fine_noise.reshape(z.pairs, z.fine, z.fine_slots),
        fine_basis,
        medium_state.transpose(0, 2, 1, 3),
        medium_noise.transpose(0, 2, 1, 3),
        medium_basis,
        coarse_state,
        coarse_noise,
        coarse_basis,
    )
    operands = tuple(pltpu.with_memory_space_constraint(x, pltpu.HBM) for x in operands)
    vmem = pl.BlockSpec(memory_space=pltpu.VMEM)
    hbm = pl.BlockSpec(memory_space=pltpu.HBM)
    smem = pl.BlockSpec(memory_space=pltpu.SMEM)
    between = (
        pltpu.VMEM((z.pairs, z.fine, z.fine_slots), f32),
        pltpu.VMEM((tiles, e, z.medium, 2, LANES), f32),
        pltpu.VMEM((2, z.coarse, z.coarse_slots), f32),
        pltpu.VMEM((2, n, SUB, LANES), bf16),
        pltpu.VMEM((lat, SUB, LANES), bf16),
        pltpu.VMEM((table_rows, 2 * z.wrap), bf16),
    )
    held = pl.pallas_call(
        functools.partial(spread_kernel, z),
        out_shape=between,
        in_specs=[smem, smem] + [hbm] * 9,
        out_specs=(vmem,) * 6,
        scratch_shapes=[
            pltpu.VMEM((z.groups, z.pairs, SUB, z.fine_slots), bf16),
            pltpu.VMEM((z.fine, rows, z.fine_slots), bf16),
            pltpu.VMEM((SUB * z.pairs, z.fine_slots), bf16),
            pltpu.VMEM((z.groups * rows, 2 * LANES), bf16),
            pltpu.VMEM((tiles, e, z.medium, 2, LANES), bf16),
            pltpu.VMEM((z.medium, rows, z.medium_slots), bf16),
            pltpu.VMEM((z.medium * z.pairs, z.medium_slots), bf16),
            pltpu.VMEM((rows * 3 * SUB, LANES), f32),
            pltpu.VMEM((2, n, SUB, LANES), bf16),
            pltpu.VMEM((2, z.coarse, z.coarse_slots), bf16),
            pltpu.VMEM((z.coarse, z.coarse_slots), bf16),
            pltpu.VMEM((lat, 32, LANES), bf16),
            pltpu.VMEM((far, 32, LANES), bf16),
            pltpu.VMEM((lat, 32, LANES), bf16),
            pltpu.VMEM((lat, 32, LANES), bf16),
            pltpu.VMEM((lat * 5 * SUB, LANES), f32),
            pltpu.VMEM((12 * lat, 2 * LANES), bf16),
            pltpu.VMEM((12 * z.pairs, 2 * LANES), bf16),
            pltpu.VMEM((lat * SUB, LANES), f32),
            pltpu.VMEM((lat, SUB, LANES), bf16),
            pltpu.VMEM((2 * n, z.wrap), f32),
            pltpu.VMEM((2 * n, z.wrap), f32),
            dma((3, z.groups)),
            dma((2 * tiles + 1,)),
            dma((3,)),
            dma((2, n)),
            dma((2, n)),
            dma((lat,)),
            dma((lat,)),
            dma((lat,)),
            dma((lat,)),
            dma((lat,)),
            dma((lat,)),
        ],
        compiler_params=pltpu.CompilerParams(
            collective_id=0, has_side_effects=True, vmem_limit_bytes=32 * 1024 * 1024
        ),
    )(decay, amplitude, *operands)
    fine_next, medium_next, coarse_next, pattern = pl.pallas_call(
        functools.partial(grid_kernel, z),
        out_shape=(
            jax.ShapeDtypeStruct((z.pairs, z.fine, z.fine_slots), f32),
            jax.ShapeDtypeStruct((e, z.medium, 2, z.medium_slots), f32),
            jax.ShapeDtypeStruct(coarse_state.shape, f32),
            jax.ShapeDtypeStruct((e * NLON // LANES, LANES), f32),
        ),
        in_specs=[vmem] * 6,
        out_specs=(hbm, hbm, hbm, vmem),
        scratch_shapes=[pltpu.VMEM((LANES, table_rows), bf16), dma((2 + tiles,))],
        compiler_params=pltpu.CompilerParams(vmem_limit_bytes=32 * 1024 * 1024),
    )(*held)
    return (
        fine_next.reshape(fine_state.shape),
        medium_next.transpose(0, 2, 1, 3),
        coarse_next,
        pattern.reshape(e, 1, NLON),
    )


def body(*arrays):
    fine_state, medium_state, coarse_state = arrays[0], arrays[2], arrays[4]
    scale, lat = lax.axis_size("scale"), lax.axis_size("lat")
    z = Sizes(fine_state, medium_state, coarse_state, arrays[8], arrays[10], scale, lat)
    return fast_body(z, *arrays) if z.fits() else general_body(*arrays)


def solution(mesh):
    return jax.shard_map(
        body,
        mesh=mesh,
        in_specs=(
            P(None, None, ("scale", "lat"), None),
            P(None, None, ("scale", "lat"), None),
            P(None, None, ("scale", "lat"), None),
            P(None, None, ("scale", "lat"), None),
            P("lat", None, None, None),
            P("lat", None, None, None),
            P(),
            P(),
            P(("scale", "lat"), None, None),
            P(("scale", "lat"), None, None),
            P(("scale", "lat"), None, None),
        ),
        out_specs=(
            P(None, None, ("scale", "lat"), None),
            P(None, None, ("scale", "lat"), None),
            P("lat", None, None, None),
            P(None, ("scale", "lat"), None),
        ),
        check_vma=False,
    )
```

```python
import functools
import math

import jax
import jax.numpy as jnp
import numpy as np
from jax import lax
from jax.experimental import pallas as pl
from jax.experimental.pallas import tpu as pltpu
from jax.sharding import PartitionSpec as P

NLON = 2560
LANES = 128
FOLD = NLON // LANES


def advance(state, noise, decay_rate, amp_rate, offset):
    slots = state.shape[3]
    mode_ids = offset + jnp.arange(state.shape[2], dtype=jnp.int32)
    degree_ids = jnp.arange(slots, dtype=jnp.int32)
    inside = mode_ids[:, None] + degree_ids[None, :] < slots
    updated = decay_rate * state + amp_rate * noise.astype(jnp.float32)
    return jnp.where(inside, updated, jnp.zeros_like(updated))


def phase_rows(block, devices):
    return max((p * block % FOLD + block - 1) // FOLD + 1 for p in range(devices))


def phase_blocks(fourier, place, devices, modes=None):
    rows, parts, block, members = fourier.shape
    high = phase_rows(block, devices)
    if block % FOLD:
        start = (place * block % FOLD).astype(jnp.int32)
        room = jnp.zeros((rows, parts, high * FOLD, members), fourier.dtype)
        zero = jnp.zeros((), jnp.int32)
        fourier = lax.dynamic_update_slice(room, fourier, (zero, zero, start, zero))
    return fourier.reshape(rows, parts * high, FOLD * members)


def received_rows(blocks, devices, width):
    source = np.arange(devices, dtype=np.int32)
    cols, parts = [], []
    for block in blocks:
        for part in range(2):
            for j in range(phase_rows(block, devices)):
                cols.append(source * block // FOLD + j)
                parts.append(part)
    while len(cols) < width:
        cols.append(source * 0)
        parts.append(0)
    high = np.stack(cols, axis=1).reshape(-1, 1)
    part = np.tile(np.array(parts, np.int32), devices)[:, None]
    return np.concatenate([high, part], axis=1).astype(np.int32)


def table_kernel(rows_ref, table_ref):
    count = rows_ref.shape[0]
    high, part = rows_ref[:, 0:1], rows_ref[:, 1:2]
    lon = lax.broadcasted_iota(jnp.int32, (count, LANES), 1)
    turns = (high * lon + part * (LANES // 4)) % LANES
    angle = turns.astype(jnp.float32) * (2.0 * math.pi / LANES)
    re, im = 2.0 * jnp.cos(angle), 2.0 * jnp.sin(angle)
    first = jnp.where(high == 0, 0.5, 1.0).astype(jnp.float32)
    shape = (-(-FOLD // 8) * 8, LANES)
    low = lax.broadcasted_iota(jnp.int32, shape, 0) * lax.broadcasted_iota(jnp.int32, shape, 1)
    low = low.astype(jnp.float32) * (2.0 * math.pi / NLON)
    cos, sin = jnp.cos(low), jnp.sin(low)
    for q in range(FOLD):
        cl, sl = cos[q : q + 1], sin[q : q + 1]
        real, imag = re * cl - im * sl, im * cl + re * sl
        if q == 0:
            real, imag = real * first, imag * first
        table_ref[q, :, :LANES] = real.astype(jnp.bfloat16)
        table_ref[q, :, LANES:] = imag.astype(jnp.bfloat16)


def longitude_kernel(members, got_ref, table_ref, out_ref):
    own = got_ref.shape[1]
    for i in range(own):
        spread = got_ref[:, i].astype(jnp.float32)
        spread = spread.reshape(spread.shape[0] * spread.shape[1], spread.shape[2])
        lanes = -spread.shape[1] % LANES
        if lanes:
            spread = jnp.concatenate(
                [spread, jnp.zeros((spread.shape[0], lanes), jnp.float32)], axis=1
            )
        turned = spread.T.astype(jnp.bfloat16)
        totals = [None] * FOLD
        for q in range(FOLD):
            part = jnp.dot(
                turned[q * members : (q + 1) * members],
                table_ref[q],
                preferred_element_type=jnp.float32,
            )
            real, imag = part[:, :LANES], part[:, LANES:]
            for h in range(FOLD):
                turn = 2.0 * math.pi * (q * h % FOLD) / FOLD
                term = math.cos(turn) * real - math.sin(turn) * imag
                totals[h] = term if q == 0 else totals[h] + term
        for h in range(FOLD):
            out_ref[:, i, h * LANES : (h + 1) * LANES] = jnp.tanh(totals[h])


def coarse_kernel(
    part_modes, decay_ref, amp_ref, state_ref, noise_ref, basis_ref, next_ref, mixed_ref, fine_ref, medium_ref
):
    held, parts, modes, slots = state_ref.shape
    for scale, rate_ref in ((0, fine_ref), (1, medium_ref)):
        rate_ref[0:1] = jnp.full((1, rate_ref.shape[1]), decay_ref[scale], jnp.float32)
        rate_ref[1:2] = jnp.full((1, rate_ref.shape[1]), amp_ref[scale], jnp.float32)
    mode_ids = lax.broadcasted_iota(jnp.int32, (modes, slots), 0)
    degree_ids = lax.broadcasted_iota(jnp.int32, (modes, slots), 1)
    inside = mode_ids + degree_ids < slots
    planes = []
    for e in range(held):
        for c in range(parts):
            new = decay_ref[2] * state_ref[e, c] + amp_ref[2] * noise_ref[e, c].astype(jnp.float32)
            new = jnp.where(inside, new, 0.0)
            next_ref[e, c] = new
            planes.append(new)
    for r in range(basis_ref.shape[0]):
        planes.append(basis_ref[r].astype(jnp.float32))
    empty = jnp.zeros((part_modes, slots), jnp.float32)
    for d in range(mixed_ref.shape[0]):
        pieces = []
        for plane in planes:
            piece = plane[d * part_modes : min((d + 1) * part_modes, modes)]
            missing = part_modes - piece.shape[0]
            if missing == part_modes:
                piece = empty
            elif missing:
                piece = jnp.concatenate([piece, empty[:missing]], axis=0)
            pieces.append(piece)
        mixed_ref[d] = jnp.concatenate(pieces, axis=0).astype(jnp.bfloat16)


def general_body(
    fine_state,
    fine_noise,
    medium_state,
    medium_noise,
    coarse_state,
    coarse_noise,
    decay,
    amplitude,
    fine_basis,
    medium_basis,
    coarse_basis,
):
    devices = lax.axis_size("scale") * lax.axis_size("lat")
    lat = lax.axis_size("lat")
    held, _, modes, slots = coarse_state.shape
    own = coarse_basis.shape[0]
    part_modes = -(-modes // devices)
    vmem = pl.BlockSpec(memory_space=pltpu.VMEM)
    smem = pl.BlockSpec(memory_space=pltpu.SMEM)
    coarse_next, mixed, fine_rates, medium_rates = pl.pallas_call(
        functools.partial(coarse_kernel, part_modes),
        out_shape=(
            jax.ShapeDtypeStruct(coarse_state.shape, jnp.float32),
            jax.ShapeDtypeStruct((devices, (2 * held + own) * part_modes, slots), jnp.bfloat16),
            jax.ShapeDtypeStruct((2, fine_state.shape[3]), jnp.float32),
            jax.ShapeDtypeStruct((2, medium_state.shape[3]), jnp.float32),
        ),
        in_specs=[smem, smem, vmem, vmem, vmem],
        out_specs=(vmem,) * 4,
    )(decay, amplitude, coarse_state, coarse_noise, coarse_basis)
    mixed = lax.all_to_all(mixed, ("scale", "lat"), split_axis=0, concat_axis=0, tiled=True)
    mixed = mixed.reshape(devices, 2 * held + own, part_modes, slots)
    coarse_half = mixed[:lat, : 2 * held].reshape(lat * held, 2, part_modes, slots)
    coarse_rows = mixed[:, 2 * held :].reshape(devices * own, part_modes, slots)
    place = lax.axis_index(("scale", "lat"))
    fine_next = advance(fine_state, fine_noise, fine_rates[0], fine_rates[1], place * fine_state.shape[2])
    medium_next = advance(
        medium_state, medium_noise, medium_rates[0], medium_rates[1], place * medium_state.shape[2]
    )
    fourier = []
    for half, basis, form in (
        (fine_next.astype(jnp.bfloat16), fine_basis, "ecmk,mrk->rcme"),
        (medium_next.astype(jnp.bfloat16), medium_basis, "ecmk,mrk->rcme"),
        (coarse_half, coarse_rows, "ecmk,rmk->rcme"),
    ):
        fourier.append(
            jnp.einsum(form, half, basis, preferred_element_type=jnp.float32).astype(jnp.bfloat16)
        )
    members = coarse_half.shape[0]
    blocks = [x.shape[2] for x in fourier]
    both = jnp.concatenate([phase_blocks(x, place, devices) for x in fourier], axis=1)
    width = -(-both.shape[1] // 8) * 8
    both = jnp.pad(both, ((0, 0), (0, width - both.shape[1]), (0, 0)))
    received = received_rows(blocks, devices, width)
    table = pl.pallas_call(
        table_kernel,
        out_shape=jax.ShapeDtypeStruct((FOLD, devices * width, 2 * LANES), jnp.bfloat16),
        in_specs=[vmem],
        out_specs=vmem,
        cost_estimate=pl.CostEstimate(
            flops=30 * FOLD * devices * width * LANES,
            bytes_accessed=8 * FOLD * devices * width * LANES,
            transcendentals=4 * devices * width * LANES,
        ),
    )(jnp.asarray(received))
    got = lax.all_to_all(both, ("scale", "lat"), split_axis=0, concat_axis=0, tiled=True)
    got = got.reshape(devices, own, width, FOLD * members)
    pattern = pl.pallas_call(
        functools.partial(longitude_kernel, members),
        out_shape=jax.ShapeDtypeStruct((members, own, NLON), jnp.float32),
        in_specs=[vmem, vmem],
        out_specs=vmem,
    )(got, table)
    return (fine_next, medium_next, coarse_next, pattern)


MESH = pl.DeviceIdType.MESH
SUB = 8


class Sizes:
    def __init__(self, fine_state, medium_state, coarse_state, fine_basis, coarse_basis, scale, lat):
        self.scale, self.lat, self.n = scale, lat, scale * lat
        _, self.parts, self.fine, self.fine_slots = fine_state.shape
        self.members = fine_state.shape[0]
        self.pairs = self.members * self.parts
        self.medium, self.medium_slots = medium_state.shape[2:]
        self.coarse, self.coarse_slots = coarse_state.shape[2:]
        self.held, self.own, self.rows = coarse_state.shape[0], coarse_basis.shape[0], fine_basis.shape[1]
        self.groups = self.fine // SUB
        self.quad = LANES // self.pairs
        self.piece = self.coarse // lat
        self.wrap = NLON // max(self.quad, 1)

    def fits(self):
        if self.pairs * 4 != LANES or self.parts != 2 or self.held != 1 or self.own != 1:
            return False
        if self.rows != self.n or self.members != self.lat or self.members != 16:
            return False
        if self.fine % SUB or self.medium % 4 or self.fine != 2 * self.medium:
            return False
        if self.fine_slots % LANES or self.medium_slots % LANES or self.coarse % self.lat:
            return False
        over = self.coarse_slots - LANES
        if self.coarse_slots != self.coarse or over <= 0 or 2 * over > LANES or over % self.lat:
            return False
        if 3 * self.piece > 32 or self.lat % 4 or LANES * self.pairs // self.lat % LANES:
            return False
        high = self.fine // 4
        return SUB <= high and high - SUB + self.medium // 4 <= SUB and self.wrap % LANES == 0


def turns(count, columns, period, index):
    lon = lax.broadcasted_iota(jnp.int32, (count, columns), 1)
    angle = ((index * lon) % period).astype(jnp.float32) * (2.0 * math.pi / period)
    return jnp.cos(angle), jnp.sin(angle)


def spread_kernel(
    z,
    decay_in,
    amp_in,
    fine_state,
    fine_noise,
    fine_basis,
    medium_state,
    medium_noise,
    medium_basis,
    coarse_state,
    coarse_noise,
    coarse_basis,
    fine_next,
    medium_next,
    coarse_next,
    got,
    got_coarse,
    table,
    noise_f,
    basis_f,
    half,
    picked,
    noise_m,
    basis_m,
    half_m,
    rows_f,
    send,
    noise_c,
    basis_c,
    spread,
    first,
    landed,
    landed_f,
    left_c,
    right_c,
    second,
    wave_cos,
    wave_sin,
    decay,
    amp,
    load_f,
    load_m,
    load_c,
    sent,
    came,
):
    n, lat = z.n, z.lat
    s, a = lax.axis_index("scale"), lax.axis_index("lat")
    me = s * lat + a
    f32, bf16 = jnp.float32, jnp.bfloat16
    mid_tiles = z.medium_slots // LANES
    fine_quads, medium_quads = z.fine // 4, z.medium // 4
    over = z.coarse_slots - LANES
    stride, pitch = 3 * SUB, 3 * SUB

    def place(p):
        return {"scale": p // lat, "lat": p % lat}

    barrier = pltpu.get_barrier_semaphore()

    def greet(i, _):
        pl.semaphore_signal(barrier, inc=1, device_id=place((me + i) % n), device_id_type=MESH)
        return 0

    lax.fori_loop(1, n, greet, 0)

    def coarse_loads():
        return (
            pltpu.make_async_copy(decay_in, decay, load_c),
            pltpu.make_async_copy(amp_in, amp, load_c),
            pltpu.make_async_copy(coarse_state.at[0], coarse_next, load_c),
            pltpu.make_async_copy(coarse_noise.at[0], noise_c, load_c),
            pltpu.make_async_copy(coarse_basis.at[0], basis_c, load_c),
        )

    def fine_loads(g):
        rows = pl.ds(pl.multiple_of(g * SUB, SUB), SUB)
        return (
            pltpu.make_async_copy(fine_state.at[:, rows, :], fine_next.at[:, rows, :], load_f.at[g]),
            pltpu.make_async_copy(fine_noise.at[:, rows, :], noise_f.at[g], load_f.at[g]),
            pltpu.make_async_copy(fine_basis.at[rows], basis_f.at[rows], load_f.at[g]),
        )

    def medium_loads():
        copies = [pltpu.make_async_copy(medium_basis, basis_m, load_m)]
        for t in range(mid_tiles):
            cols = pl.ds(t * LANES, LANES)
            copies.append(
                pltpu.make_async_copy(medium_state.at[:, :, :, cols], medium_next.at[t], load_m)
            )
            copies.append(
                pltpu.make_async_copy(medium_noise.at[:, :, :, cols], noise_m.at[t], load_m)
            )
        return copies

    def start(copies):
        for copy in copies:
            copy.start()

    @jax.named_scope("advance_coarse")
    def advance_coarse():
        with jax.named_scope("wait_coarse"):
            for copy in coarse_loads():
                copy.wait()
        mode = lax.broadcasted_iota(jnp.int32, (z.coarse, z.coarse_slots), 0)
        degree = lax.broadcasted_iota(jnp.int32, (z.coarse, z.coarse_slots), 1)
        inside = mode + degree < z.coarse_slots
        planes = []
        for c in range(2):
            new = decay[2] * coarse_next[c] + amp[2] * noise_c[c].astype(f32)
            new = jnp.where(inside, new, 0.0)
            coarse_next[c] = new
            planes.append(new)
        planes.append(basis_c[...].astype(f32))
        column_c = lax.broadcasted_iota(jnp.int32, (lat, LANES), 1)
        for k, plane in enumerate(planes):
            rest = plane[:over, LANES:]
            rest = jnp.concatenate([jnp.zeros_like(rest), rest, jnp.zeros((over, LANES - 2 * over), f32)], axis=1)
            for i in range(z.piece):
                rows = plane[i * lat : (i + 1) * lat, :LANES]
                low = i * lat - LANES
                if low >= 0:
                    rows = jnp.where(column_c < over, rows, rest[low : low + lat])
                spread[pl.ds((3 * i + k) * pitch, lat), :] = rows
        for p in range(lat):
            first[p] = spread[pl.ds(p, 32, stride=pitch), :].astype(bf16)

    def first_copy(p, count=None):
        at = p if count is None else pl.ds(p, count)
        to = a if count is None else at
        return pltpu.make_async_remote_copy(
            first.at[at], landed.at[to], sent.at[0], came.at[0],
            device_id={"scale": s, "lat": p}, device_id_type=MESH,
        )

    def second_copy(p, count=None):
        at = p if count is None else pl.ds(p, count)
        to = a if count is None else at
        return pltpu.make_async_remote_copy(
            second.at[at], got_coarse.at[to], sent.at[1], came.at[1],
            device_id={"scale": s, "lat": p}, device_id_type=MESH,
        )

    def row_copy(p, count=None):
        at = p if count is None else pl.ds(p, count)
        to = me if count is None else at
        return pltpu.make_async_remote_copy(
            send.at[at], got.at[to], sent.at[2], came.at[2],
            device_id=place(p), device_id_type=MESH,
        )

    lane = lax.broadcasted_iota(jnp.int32, (z.rows, 2 * LANES), 1) % SUB
    shift = lax.broadcasted_iota(jnp.int32, (SUB, z.fine_slots), 0)
    slack = z.fine_slots - me * z.fine - shift - lax.broadcasted_iota(jnp.int32, (SUB, z.fine_slots), 1)

    @jax.named_scope("fine_group")
    def fine_group(g, _):
        for copy in fine_loads(g):
            copy.wait()
        rows = pl.ds(pl.multiple_of(g * SUB, SUB), SUB)
        keep = slack > g * SUB

        def pair(i, _):
            new = decay[0] * fine_next[pl.ds(2 * i, 2), rows, :] + amp[0] * noise_f[g, pl.ds(2 * i, 2)].astype(f32)
            new = jnp.where(keep[None], new, 0.0)
            fine_next[pl.ds(2 * i, 2), rows, :] = new
            at = pl.ds(pl.multiple_of(2 * SUB * i, 2 * SUB), 2 * SUB)
            half[at, :] = new.reshape(2 * SUB, z.fine_slots).astype(bf16)
            return 0

        lax.fori_loop(0, z.pairs // 2, pair, 0)
        basis = basis_f[rows].reshape(SUB * z.rows, z.fine_slots)
        all_pairs = lax.dot_general(basis, half[...], (((1,), (1,)), ((), ())), preferred_element_type=f32)
        total = all_pairs[: z.rows]
        for q in range(1, SUB):
            total = jnp.where(lane == q, all_pairs[q * z.rows : (q + 1) * z.rows], total)
        picked[pl.ds(pl.multiple_of(g * z.rows, z.rows), z.rows), :] = total.astype(bf16)
        return 0

    target = lax.broadcasted_iota(jnp.int32, (2 * LANES, 2 * LANES), 1)
    wanted = (target % z.members) * (2 * SUB) + (target // z.members % 2) * SUB
    wanted = wanted + target // LANES * 4 + target // z.pairs % 4
    order = (lax.broadcasted_iota(jnp.int32, (2 * LANES, 2 * LANES), 0) == wanted).astype(f32).astype(bf16)
    @jax.named_scope("put_fine")
    def put_fine(g0, g1):
        moved = jnp.dot(picked[g0 * z.rows : g1 * z.rows, :], order, preferred_element_type=f32)
        for g in range(g0, g1):
            for q in range(2):
                rows_f[pl.ds(2 * g + q, z.rows, stride=stride), :] = moved[
                    (g - g0) * z.rows : (g - g0 + 1) * z.rows, q * LANES : (q + 1) * LANES
                ]

    line = lax.broadcasted_iota(jnp.int32, (SUB, LANES), 0)
    column = lax.broadcasted_iota(jnp.int32, (SUB, LANES), 1)

    def weight(row, index):
        at_zero = (line == row) & (column < z.pairs) & (index == 0)
        return jnp.where(at_zero, 0.5, 1.0).astype(f32)

    @jax.named_scope("ship")
    def ship():
        scale_row = jnp.concatenate([weight(0, me), weight(fine_quads - SUB, me)], axis=0)

        def cast(r, _):
            at = pl.ds(pl.multiple_of(r * stride, SUB), 2 * SUB)
            send[r] = (rows_f[at, :].astype(bf16).astype(f32) * scale_row).astype(bf16)
            return 0

        lax.fori_loop(0, z.rows, cast, 0, unroll=4)
        for i in range(1, n):
            row_copy((me + i) % n).start()
        got[me] = send[me]

    @jax.named_scope("send_first")
    def send_first():
        for i in range(1, lat):
            first_copy((a + i) % lat).start()
        landed[a] = first[a]

    @jax.named_scope("medium_rows")
    def medium_rows():
        for copy in medium_loads():
            copy.wait()
        flat_next = medium_next.reshape(mid_tiles * z.pairs * z.medium, LANES)
        flat_noise = noise_m.reshape(mid_tiles * z.pairs * z.medium, LANES)
        span = 2 * z.medium
        room = z.medium_slots - me * z.medium - lax.broadcasted_iota(jnp.int32, (span, LANES), 0) // 2
        room = room - lax.broadcasted_iota(jnp.int32, (span, LANES), 1)

        def medium_member(e, _):
            for t in range(mid_tiles):
                at = pl.ds(pl.multiple_of((t * z.members + e) * span, SUB), span)
                new = decay[1] * flat_next[at, :] + amp[1] * flat_noise[at, :].astype(f32)
                flat_next[at, :] = jnp.where(room > t * LANES, new, 0.0)
            return 0

        lax.fori_loop(0, z.members, medium_member, 0)

        def medium_mode(m, _):
            for c in range(2):
                at = pl.ds(pl.multiple_of(m * z.pairs + c * z.members, z.members), z.members)
                for t in range(mid_tiles):
                    new = flat_next[pl.ds(t * z.members * span + 2 * m + c, z.members, stride=span), :]
                    half_m[at, t * LANES : (t + 1) * LANES] = new.astype(bf16)
            return 0

        lax.fori_loop(0, z.medium, medium_mode, 0)
        lane4 = lax.broadcasted_iota(jnp.int32, (z.rows, LANES), 1) // z.pairs
        for q in range(medium_quads):
            basis = basis_m[4 * q : 4 * q + 4].reshape(4 * z.rows, z.medium_slots)
            all_pairs = lax.dot_general(
                basis, half_m[q * LANES : (q + 1) * LANES, :], (((1,), (1,)), ((), ())), preferred_element_type=f32
            )
            total = all_pairs[: z.rows]
            for b in range(1, 4):
                total = jnp.where(lane4 == b, all_pairs[b * z.rows : (b + 1) * z.rows], total)
            rows_f[pl.ds(fine_quads + q, z.rows, stride=stride), :] = total
        for spare in range(fine_quads + medium_quads, 2 * SUB):
            rows_f[pl.ds(spare, z.rows, stride=stride), :] = jnp.zeros((z.rows, LANES), f32)

    @jax.named_scope("wait_first")
    def wait_first():
        first_copy(0, lat - 1).wait()

    @jax.named_scope("coarse_rows")
    def coarse_rows():
        jump = 5 * SUB

        def widen(p, _):
            landed_f[pl.ds(pl.multiple_of(p * jump, SUB), 32), :] = landed[p].astype(f32)
            return 0

        lax.fori_loop(0, lat, widen, 0, unroll=4)
        lane = lax.broadcasted_iota(jnp.int32, (lat, LANES), 1)
        shared = LANES // lat
        for i in range(z.piece):
            for c in range(2):
                values = landed_f[pl.ds(3 * i + c, lat, stride=jump), :]
                right_c[i * z.pairs + c * z.members : i * z.pairs + (c + 1) * z.members, :] = values.astype(bf16)
            values = landed_f[pl.ds(3 * i + 2, lat, stride=jump), :]
            if i >= shared:
                extra = jnp.where(lane >= over, values, 0.0)
                values = jnp.where(lane < over, values, 0.0)
                left_c[(z.piece + i - shared) * lat : (z.piece + i - shared + 1) * lat, :] = extra.astype(bf16)
            left_c[i * lat : (i + 1) * lat, :] = values.astype(bf16)
        all_pairs = lax.dot_general(
            left_c[...], right_c[...], (((1,), (1,)), ((), ())), preferred_element_type=f32
        )
        slot = lax.broadcasted_iota(jnp.int32, (lat, z.piece * z.pairs), 1) // z.pairs
        total = all_pairs[:lat]
        for i in range(1, z.piece):
            total = jnp.where(slot == i, all_pairs[i * lat : (i + 1) * lat], total)
        extra = all_pairs[z.piece * lat : (z.piece + 1) * lat]
        for i in range(shared + 1, z.piece):
            extra = jnp.where(slot == i, all_pairs[(z.piece + i - shared) * lat : (z.piece + i - shared + 1) * lat], extra)
        block = lane // z.pairs
        for i in range(z.piece):
            j = i // 4
            row = total[:, j * LANES : min((j + 1) * LANES, total.shape[1])]
            if i < z.piece - shared:
                far = extra[:, shared * z.pairs + j * LANES :]
                row = row + jnp.concatenate([far, jnp.zeros((lat, LANES - far.shape[1]), f32)], axis=1)
            if row.shape[1] < LANES:
                row = jnp.concatenate([row, jnp.zeros((lat, LANES - row.shape[1]), f32)], axis=1)
            row = pltpu.roll(row, ((a % 4 - i % 4 + 4) % 4) * z.pairs, axis=1)
            spread[pl.ds(i, lat, stride=pitch), :] = jnp.where(block == a % 4, row, 0.0)
        for i in range(z.piece, 2 * SUB):
            spread[pl.ds(i, lat, stride=pitch), :] = jnp.zeros((lat, LANES), f32)
        scale_row = jnp.concatenate([weight(0, a), jnp.ones((SUB, LANES), f32)], axis=0)
        for p in range(lat):
            rows = spread[p * pitch : p * pitch + 2 * SUB, :].astype(bf16).astype(f32)
            second[p] = (rows * scale_row).astype(bf16)
        for i in range(1, lat):
            second_copy((a + i) % lat).start()
        got_coarse[a] = second[a]

    line_t = lax.broadcasted_iota(jnp.int32, (SUB, z.wrap), 0)
    left_over = fine_quads - SUB

    def twice(index):
        cos, sin = turns(SUB, z.wrap, z.wrap, index)
        return 2.0 * cos, 2.0 * sin

    def turned(base, cos, sin):
        return base[0] * cos - base[1] * sin, base[0] * sin + base[1] * cos

    def keep_rows(at, upper, lower):
        for part in range(2):
            both = jnp.concatenate([upper[part], lower[part]], axis=0).astype(bf16)
            for t in range(z.wrap // LANES):
                lo = (2 * t + part) * LANES
                table[at, lo : lo + LANES] = both[:, t * LANES : (t + 1) * LANES]

    @jax.named_scope("start_table")
    def start_table():
        count = 2 * n
        step = medium_quads * lax.broadcasted_iota(jnp.int32, (count, z.wrap), 0)
        wave_cos[...], wave_sin[...] = turns(count, z.wrap, z.wrap, step)

    def wave(u):
        return wave_cos[pl.ds(u, 1), :], wave_sin[pl.ds(u, 1), :]

    @jax.named_scope("fill_table")
    def fill_table(lo, hi):
        base = twice(line_t)
        mixed = twice(jnp.where(line_t < left_over, SUB + line_t, line_t - left_over))

        def fill_rows(p, _):
            cos, sin = wave(2 * p)
            upper = turned(base, cos, sin)
            low_cos, low_sin = wave(p)
            cos = jnp.where(line_t < left_over, cos, low_cos)
            sin = jnp.where(line_t < left_over, sin, low_sin)
            at = pl.multiple_of(2 * SUB * p, 2 * SUB)
            keep_rows(pl.ds(at, 2 * SUB), upper, turned(mixed, cos, sin))
            return 0

        lax.fori_loop(lo, hi, fill_rows, 0)

    @jax.named_scope("end_table")
    def end_table():
        upper, lower = twice(4 * line_t), twice(4 * (SUB + line_t))
        for u in range(4):
            cos, sin = turns(1, z.wrap, z.wrap, u)
            at = 2 * SUB * (n + u)
            keep_rows(slice(at, at + 2 * SUB), turned(upper, cos, sin), turned(lower, cos, sin))

    @jax.named_scope("collect")
    def collect():
        row_copy(0, n - 1).wait()
        second_copy(0, lat - 1).wait()

    @jax.named_scope("meet")
    def meet():
        pl.semaphore_wait(barrier, n - 1)

    start(coarse_loads())
    start(fine_loads(0))
    start_table()
    start(fine_loads(1))
    fill_table(0, n // 2)
    start(fine_loads(2))
    fill_table(n // 2, n)
    end_table()
    start(fine_loads(3))
    advance_coarse()
    lax.fori_loop(0, 1, fine_group, 0)
    start(medium_loads())
    meet()
    send_first()
    lax.fori_loop(1, 2, fine_group, 0)
    start(fine_loads(z.groups - 1))
    lax.fori_loop(2, z.groups - 1, fine_group, 0)
    put_fine(0, z.groups - 1)
    medium_rows()
    lax.fori_loop(z.groups - 1, z.groups, fine_group, 0)
    put_fine(z.groups - 1, z.groups)
    ship()
    wait_first()
    coarse_rows()
    collect()


def grid_kernel(
    z, fine_in, medium_in, coarse_in, got, got_coarse, table, fine_out, medium_out, coarse_out, out, turned, sems
):
    copies = [
        pltpu.make_async_copy(fine_in, fine_out, sems.at[0]),
        pltpu.make_async_copy(coarse_in, coarse_out.at[0], sems.at[1]),
    ]
    for t in range(medium_in.shape[0]):
        cols = pl.ds(t * LANES, LANES)
        copies.append(pltpu.make_async_copy(medium_in.at[t], medium_out.at[:, :, :, cols], sems.at[2 + t]))
    for copy in copies:
        copy.start()
    many = 2 * z.n * SUB
    fours = z.lat // 4
    turned[:, :many] = got[...].reshape(many, LANES).astype(jnp.float32).T.astype(jnp.bfloat16)
    few = got_coarse[...].astype(jnp.float32).reshape(fours, 4, 2 * SUB, LANES)
    few = (few[:, 0] + few[:, 1] + few[:, 2] + few[:, 3]).reshape(fours * 2 * SUB, LANES)
    turned[:, many:] = few.T.astype(jnp.bfloat16)
    e, tiles = z.members, z.wrap // LANES
    for t in range(tiles):
        both = jnp.dot(turned[...], table[:, 2 * t * LANES : 2 * (t + 1) * LANES], preferred_element_type=jnp.float32)
        waves = []
        for b in range(4):
            at = 2 * b * e
            cos_r, sin_r = both[at : at + e, :LANES], both[at : at + e, LANES:]
            cos_i, sin_i = both[at + e : at + 2 * e, :LANES], both[at + e : at + 2 * e, LANES:]
            re, im = cos_r - sin_i, sin_r + cos_i
            if b:
                angle = (lax.broadcasted_iota(jnp.int32, (1, LANES), 1) + t * LANES).astype(jnp.float32)
                angle = angle * (2.0 * math.pi * b / NLON)
                cos, sin = jnp.cos(angle), jnp.sin(angle)
                re, im = re * cos - im * sin, re * sin + im * cos
            waves.append((re, im))
        for h in range(4):
            total = None
            for b in range(4):
                re, im = waves[b]
                term = (re, -im, -re, im)[b * h % 4]
                total = term if total is None else total + term
            out[pl.ds(h * tiles + t, e, stride=4 * tiles), :] = jnp.tanh(total)
    for copy in copies:
        copy.wait()


def fast_body(
    z,
    fine_state,
    fine_noise,
    medium_state,
    medium_noise,
    coarse_state,
    coarse_noise,
    decay,
    amplitude,
    fine_basis,
    medium_basis,
    coarse_basis,
):
    f32, bf16, dma = jnp.float32, jnp.bfloat16, pltpu.SemaphoreType.DMA
    e, n, lat, rows = z.members, z.n, z.lat, z.rows
    tiles = z.medium_slots // LANES
    shared = z.piece - LANES // lat
    table_rows = (n + lat // 4) * 2 * SUB
    operands = (
        decay,
        amplitude,
        fine_state.reshape(z.pairs, z.fine, z.fine_slots),
        fine_noise.reshape(z.pairs, z.fine, z.fine_slots),
        fine_basis,
        medium_state.transpose(0, 2, 1, 3),
        medium_noise.transpose(0, 2, 1, 3),
        medium_basis,
        coarse_state,
        coarse_noise,
        coarse_basis,
    )
    operands = tuple(pltpu.with_memory_space_constraint(x, pltpu.HBM) for x in operands)
    vmem = pl.BlockSpec(memory_space=pltpu.VMEM)
    hbm = pl.BlockSpec(memory_space=pltpu.HBM)
    between = (
        pltpu.VMEM((z.pairs, z.fine, z.fine_slots), f32),
        pltpu.VMEM((tiles, e, z.medium, 2, LANES), f32),
        pltpu.VMEM((2, z.coarse, z.coarse_slots), f32),
        pltpu.VMEM((n, 2 * SUB, LANES), bf16),
        pltpu.VMEM((lat, 2 * SUB, LANES), bf16),
        pltpu.VMEM((table_rows, 2 * z.wrap), bf16),
    )
    held = pl.pallas_call(
        functools.partial(spread_kernel, z),
        out_shape=between,
        in_specs=[hbm] * 11,
        out_specs=(vmem,) * 6,
        scratch_shapes=[
            pltpu.VMEM((z.groups, z.pairs, SUB, z.fine_slots), bf16),
            pltpu.VMEM((z.fine, rows, z.fine_slots), bf16),
            pltpu.VMEM((SUB * z.pairs, z.fine_slots), bf16),
            pltpu.VMEM((z.groups * rows, 2 * LANES), bf16),
            pltpu.VMEM((tiles, e, z.medium, 2, LANES), bf16),
            pltpu.VMEM((z.medium, rows, z.medium_slots), bf16),
            pltpu.VMEM((z.medium * z.pairs, z.medium_slots), bf16),
            pltpu.VMEM((rows * 3 * SUB, LANES), f32),
            pltpu.VMEM((n, 2 * SUB, LANES), bf16),
            pltpu.VMEM((2, z.coarse, z.coarse_slots), bf16),
            pltpu.VMEM((z.coarse, z.coarse_slots), bf16),
            pltpu.VMEM((32 * 3 * SUB, LANES), f32),
            pltpu.VMEM((lat, 32, LANES), bf16),
            pltpu.VMEM((lat, 32, LANES), bf16),
            pltpu.VMEM((lat * 5 * SUB, LANES), f32),
            pltpu.VMEM(((z.piece + shared) * lat, LANES), bf16),
            pltpu.VMEM((z.piece * z.pairs, LANES), bf16),
            pltpu.VMEM((lat, 2 * SUB, LANES), bf16),
            pltpu.VMEM((2 * n, z.wrap), f32),
            pltpu.VMEM((2 * n, z.wrap), f32),
            pltpu.SMEM((3,), f32),
            pltpu.SMEM((3,), f32),
            dma((z.groups,)),
            dma,
            dma,
            dma((3,)),
            dma((3,)),
        ],
        compiler_params=pltpu.CompilerParams(
            collective_id=0, has_side_effects=True, vmem_limit_bytes=32 * 1024 * 1024
        ),
    )(*operands)
    fine_next, medium_next, coarse_next, pattern = pl.pallas_call(
        functools.partial(grid_kernel, z),
        out_shape=(
            jax.ShapeDtypeStruct((z.pairs, z.fine, z.fine_slots), f32),
            jax.ShapeDtypeStruct((e, z.medium, 2, z.medium_slots), f32),
            jax.ShapeDtypeStruct(coarse_state.shape, f32),
            jax.ShapeDtypeStruct((e * NLON // LANES, LANES), f32),
        ),
        in_specs=[vmem] * 6,
        out_specs=(hbm, hbm, hbm, vmem),
        scratch_shapes=[pltpu.VMEM((LANES, table_rows), bf16), dma((2 + tiles,))],
        compiler_params=pltpu.CompilerParams(vmem_limit_bytes=32 * 1024 * 1024),
    )(*held)
    return (
        fine_next.reshape(fine_state.shape),
        medium_next.transpose(0, 2, 1, 3),
        coarse_next,
        pattern.reshape(e, 1, NLON),
    )


def body(*arrays):
    fine_state, medium_state, coarse_state = arrays[0], arrays[2], arrays[4]
    scale, lat = lax.axis_size("scale"), lax.axis_size("lat")
    z = Sizes(fine_state, medium_state, coarse_state, arrays[8], arrays[10], scale, lat)
    return fast_body(z, *arrays) if z.fits() else general_body(*arrays)


def solution(mesh):
    return jax.shard_map(
        body,
        mesh=mesh,
        in_specs=(
            P(None, None, ("scale", "lat"), None),
            P(None, None, ("scale", "lat"), None),
            P(None, None, ("scale", "lat"), None),
            P(None, None, ("scale", "lat"), None),
            P("lat", None, None, None),
            P("lat", None, None, None),
            P(),
            P(),
            P(("scale", "lat"), None, None),
            P(("scale", "lat"), None, None),
            P(("scale", "lat"), None, None),
        ),
        out_specs=(
            P(None, None, ("scale", "lat"), None),
            P(None, None, ("scale", "lat"), None),
            P("lat", None, None, None),
            P(None, ("scale", "lat"), None),
        ),
        check_vma=False,
    )
```

```python
import functools
import math

import jax
import jax.numpy as jnp
import numpy as np
from jax import lax
from jax.experimental import pallas as pl
from jax.experimental.pallas import tpu as pltpu
from jax.sharding import PartitionSpec as P

NLON = 2560
LANES = 128
FOLD = NLON // LANES


def advance(state, noise, decay_rate, amp_rate, offset):
    slots = state.shape[3]
    mode_ids = offset + jnp.arange(state.shape[2], dtype=jnp.int32)
    degree_ids = jnp.arange(slots, dtype=jnp.int32)
    inside = mode_ids[:, None] + degree_ids[None, :] < slots
    updated = decay_rate * state + amp_rate * noise.astype(jnp.float32)
    return jnp.where(inside, updated, jnp.zeros_like(updated))


def phase_rows(block, devices):
    return max((p * block % FOLD + block - 1) // FOLD + 1 for p in range(devices))


def phase_blocks(fourier, place, devices, modes=None):
    rows, parts, block, members = fourier.shape
    high = phase_rows(block, devices)
    if block % FOLD:
        start = (place * block % FOLD).astype(jnp.int32)
        room = jnp.zeros((rows, parts, high * FOLD, members), fourier.dtype)
        zero = jnp.zeros((), jnp.int32)
        fourier = lax.dynamic_update_slice(room, fourier, (zero, zero, start, zero))
    return fourier.reshape(rows, parts * high, FOLD * members)


def received_rows(blocks, devices, width):
    source = np.arange(devices, dtype=np.int32)
    cols, parts = [], []
    for block in blocks:
        for part in range(2):
            for j in range(phase_rows(block, devices)):
                cols.append(source * block // FOLD + j)
                parts.append(part)
    while len(cols) < width:
        cols.append(source * 0)
        parts.append(0)
    high = np.stack(cols, axis=1).reshape(-1, 1)
    part = np.tile(np.array(parts, np.int32), devices)[:, None]
    return np.concatenate([high, part], axis=1).astype(np.int32)


def table_kernel(rows_ref, table_ref):
    count = rows_ref.shape[0]
    high, part = rows_ref[:, 0:1], rows_ref[:, 1:2]
    lon = lax.broadcasted_iota(jnp.int32, (count, LANES), 1)
    turns = (high * lon + part * (LANES // 4)) % LANES
    angle = turns.astype(jnp.float32) * (2.0 * math.pi / LANES)
    re, im = 2.0 * jnp.cos(angle), 2.0 * jnp.sin(angle)
    first = jnp.where(high == 0, 0.5, 1.0).astype(jnp.float32)
    shape = (-(-FOLD // 8) * 8, LANES)
    low = lax.broadcasted_iota(jnp.int32, shape, 0) * lax.broadcasted_iota(jnp.int32, shape, 1)
    low = low.astype(jnp.float32) * (2.0 * math.pi / NLON)
    cos, sin = jnp.cos(low), jnp.sin(low)
    for q in range(FOLD):
        cl, sl = cos[q : q + 1], sin[q : q + 1]
        real, imag = re * cl - im * sl, im * cl + re * sl
        if q == 0:
            real, imag = real * first, imag * first
        table_ref[q, :, :LANES] = real.astype(jnp.bfloat16)
        table_ref[q, :, LANES:] = imag.astype(jnp.bfloat16)


def longitude_kernel(members, got_ref, table_ref, out_ref):
    own = got_ref.shape[1]
    for i in range(own):
        spread = got_ref[:, i].astype(jnp.float32)
        spread = spread.reshape(spread.shape[0] * spread.shape[1], spread.shape[2])
        lanes = -spread.shape[1] % LANES
        if lanes:
            spread = jnp.concatenate(
                [spread, jnp.zeros((spread.shape[0], lanes), jnp.float32)], axis=1
            )
        turned = spread.T.astype(jnp.bfloat16)
        totals = [None] * FOLD
        for q in range(FOLD):
            part = jnp.dot(
                turned[q * members : (q + 1) * members],
                table_ref[q],
                preferred_element_type=jnp.float32,
            )
            real, imag = part[:, :LANES], part[:, LANES:]
            for h in range(FOLD):
                turn = 2.0 * math.pi * (q * h % FOLD) / FOLD
                term = math.cos(turn) * real - math.sin(turn) * imag
                totals[h] = term if q == 0 else totals[h] + term
        for h in range(FOLD):
            out_ref[:, i, h * LANES : (h + 1) * LANES] = jnp.tanh(totals[h])


def coarse_kernel(
    part_modes, decay_ref, amp_ref, state_ref, noise_ref, basis_ref, next_ref, mixed_ref, fine_ref, medium_ref
):
    held, parts, modes, slots = state_ref.shape
    for scale, rate_ref in ((0, fine_ref), (1, medium_ref)):
        rate_ref[0:1] = jnp.full((1, rate_ref.shape[1]), decay_ref[scale], jnp.float32)
        rate_ref[1:2] = jnp.full((1, rate_ref.shape[1]), amp_ref[scale], jnp.float32)
    mode_ids = lax.broadcasted_iota(jnp.int32, (modes, slots), 0)
    degree_ids = lax.broadcasted_iota(jnp.int32, (modes, slots), 1)
    inside = mode_ids + degree_ids < slots
    planes = []
    for e in range(held):
        for c in range(parts):
            new = decay_ref[2] * state_ref[e, c] + amp_ref[2] * noise_ref[e, c].astype(jnp.float32)
            new = jnp.where(inside, new, 0.0)
            next_ref[e, c] = new
            planes.append(new)
    for r in range(basis_ref.shape[0]):
        planes.append(basis_ref[r].astype(jnp.float32))
    empty = jnp.zeros((part_modes, slots), jnp.float32)
    for d in range(mixed_ref.shape[0]):
        pieces = []
        for plane in planes:
            piece = plane[d * part_modes : min((d + 1) * part_modes, modes)]
            missing = part_modes - piece.shape[0]
            if missing == part_modes:
                piece = empty
            elif missing:
                piece = jnp.concatenate([piece, empty[:missing]], axis=0)
            pieces.append(piece)
        mixed_ref[d] = jnp.concatenate(pieces, axis=0).astype(jnp.bfloat16)


def general_body(
    fine_state,
    fine_noise,
    medium_state,
    medium_noise,
    coarse_state,
    coarse_noise,
    decay,
    amplitude,
    fine_basis,
    medium_basis,
    coarse_basis,
):
    devices = lax.axis_size("scale") * lax.axis_size("lat")
    lat = lax.axis_size("lat")
    held, _, modes, slots = coarse_state.shape
    own = coarse_basis.shape[0]
    part_modes = -(-modes // devices)
    vmem = pl.BlockSpec(memory_space=pltpu.VMEM)
    smem = pl.BlockSpec(memory_space=pltpu.SMEM)
    coarse_next, mixed, fine_rates, medium_rates = pl.pallas_call(
        functools.partial(coarse_kernel, part_modes),
        out_shape=(
            jax.ShapeDtypeStruct(coarse_state.shape, jnp.float32),
            jax.ShapeDtypeStruct((devices, (2 * held + own) * part_modes, slots), jnp.bfloat16),
            jax.ShapeDtypeStruct((2, fine_state.shape[3]), jnp.float32),
            jax.ShapeDtypeStruct((2, medium_state.shape[3]), jnp.float32),
        ),
        in_specs=[smem, smem, vmem, vmem, vmem],
        out_specs=(vmem,) * 4,
    )(decay, amplitude, coarse_state, coarse_noise, coarse_basis)
    mixed = lax.all_to_all(mixed, ("scale", "lat"), split_axis=0, concat_axis=0, tiled=True)
    mixed = mixed.reshape(devices, 2 * held + own, part_modes, slots)
    coarse_half = mixed[:lat, : 2 * held].reshape(lat * held, 2, part_modes, slots)
    coarse_rows = mixed[:, 2 * held :].reshape(devices * own, part_modes, slots)
    place = lax.axis_index(("scale", "lat"))
    fine_next = advance(fine_state, fine_noise, fine_rates[0], fine_rates[1], place * fine_state.shape[2])
    medium_next = advance(
        medium_state, medium_noise, medium_rates[0], medium_rates[1], place * medium_state.shape[2]
    )
    fourier = []
    for half, basis, form in (
        (fine_next.astype(jnp.bfloat16), fine_basis, "ecmk,mrk->rcme"),
        (medium_next.astype(jnp.bfloat16), medium_basis, "ecmk,mrk->rcme"),
        (coarse_half, coarse_rows, "ecmk,rmk->rcme"),
    ):
        fourier.append(
            jnp.einsum(form, half, basis, preferred_element_type=jnp.float32).astype(jnp.bfloat16)
        )
    members = coarse_half.shape[0]
    blocks = [x.shape[2] for x in fourier]
    both = jnp.concatenate([phase_blocks(x, place, devices) for x in fourier], axis=1)
    width = -(-both.shape[1] // 8) * 8
    both = jnp.pad(both, ((0, 0), (0, width - both.shape[1]), (0, 0)))
    received = received_rows(blocks, devices, width)
    table = pl.pallas_call(
        table_kernel,
        out_shape=jax.ShapeDtypeStruct((FOLD, devices * width, 2 * LANES), jnp.bfloat16),
        in_specs=[vmem],
        out_specs=vmem,
        cost_estimate=pl.CostEstimate(
            flops=30 * FOLD * devices * width * LANES,
            bytes_accessed=8 * FOLD * devices * width * LANES,
            transcendentals=4 * devices * width * LANES,
        ),
    )(jnp.asarray(received))
    got = lax.all_to_all(both, ("scale", "lat"), split_axis=0, concat_axis=0, tiled=True)
    got = got.reshape(devices, own, width, FOLD * members)
    pattern = pl.pallas_call(
        functools.partial(longitude_kernel, members),
        out_shape=jax.ShapeDtypeStruct((members, own, NLON), jnp.float32),
        in_specs=[vmem, vmem],
        out_specs=vmem,
    )(got, table)
    return (fine_next, medium_next, coarse_next, pattern)


MESH = pl.DeviceIdType.MESH
SUB = 8


class Sizes:
    def __init__(self, fine_state, medium_state, coarse_state, fine_basis, coarse_basis, scale, lat):
        self.scale, self.lat, self.n = scale, lat, scale * lat
        _, self.parts, self.fine, self.fine_slots = fine_state.shape
        self.members = fine_state.shape[0]
        self.pairs = self.members * self.parts
        self.medium, self.medium_slots = medium_state.shape[2:]
        self.coarse, self.coarse_slots = coarse_state.shape[2:]
        self.held, self.own, self.rows = coarse_state.shape[0], coarse_basis.shape[0], fine_basis.shape[1]
        self.groups = self.fine // SUB
        self.quad = LANES // self.pairs
        self.medium_room = self.medium + 1
        self.quarter, self.owners = lat // 4, lat // 2
        self.piece = self.coarse // max(self.owners, 1)
        self.low = LANES // max(self.owners, 1)
        self.first_rows = -(-3 * self.low // SUB) * SUB
        self.wrap = NLON // max(self.quad, 1)

    def fits(self):
        if self.pairs * 4 != LANES or self.parts != 2 or self.held != 1 or self.own != 1:
            return False
        if self.rows != self.n or self.members != self.lat or self.members != 16:
            return False
        if self.fine % SUB or self.medium % 4 or self.fine != 2 * self.medium:
            return False
        if self.fine_slots % (2 * LANES) or self.medium_slots % LANES or self.scale != 2:
            return False
        over = self.coarse_slots - LANES
        if self.coarse_slots != self.coarse or 4 * over != LANES or over % self.owners:
            return False
        if self.owners != SUB or self.coarse % self.owners or over // self.owners != 4 or self.low % 4 or self.piece > 4 * SUB:
            return False
        if self.n * self.fine > self.fine_slots or self.n * self.medium > self.medium_slots:
            return False
        high = self.fine // 4
        return SUB <= high and high - SUB + self.medium // 4 <= SUB and self.wrap % LANES == 0


def turns(count, columns, period, index):
    lon = lax.broadcasted_iota(jnp.int32, (count, columns), 1)
    angle = ((index * lon) % period).astype(jnp.float32) * (2.0 * math.pi / period)
    return jnp.cos(angle), jnp.sin(angle)


def spread_kernel(
    z,
    decay_in,
    amp_in,
    fine_state,
    fine_noise,
    fine_basis,
    medium_state,
    medium_noise,
    medium_basis,
    coarse_state,
    coarse_noise,
    coarse_basis,
    fine_next,
    medium_next,
    coarse_next,
    got,
    got_coarse,
    table,
    noise_f,
    basis_f,
    half,
    picked,
    noise_m,
    basis_m,
    half_m,
    picked_m,
    rows_f,
    send,
    noise_c,
    basis_c,
    spread,
    first,
    landed,
    landed_f,
    left_c,
    right_c,
    second,
    wave_cos,
    wave_sin,
    decay,
    amp,
    load_f,
    load_m,
    load_c,
    sent,
    came,
    twin,
):
    n, lat = z.n, z.lat
    s, a = lax.axis_index("scale"), lax.axis_index("lat")
    me = s * lat + a
    f32, bf16 = jnp.float32, jnp.bfloat16
    mid_tiles = z.medium_slots // LANES
    fine_quads, medium_quads = z.fine // 4, z.medium // 4
    over = z.coarse_slots - LANES
    stride, pitch = 3 * SUB, 3 * SUB

    def place(p):
        return {"scale": p // lat, "lat": p % lat}

    barrier = pltpu.get_barrier_semaphore()

    quarter, owners = z.quarter, z.owners
    owner = (a >= quarter) & (a < quarter + owners)
    mine = jnp.where(owner, a - quarter, 0)

    def greet():
        for i in range(1, lat):
            near = {"scale": s, "lat": (a + i) % lat}
            pl.semaphore_signal(barrier, inc=1, device_id=near, device_id_type=MESH)
        pl.semaphore_signal(barrier, inc=1, device_id={"scale": 1 - s, "lat": a}, device_id_type=MESH)

    def coarse_loads():
        return (
            pltpu.make_async_copy(decay_in, decay, load_c),
            pltpu.make_async_copy(amp_in, amp, load_c),
            pltpu.make_async_copy(coarse_state.at[0], coarse_next, load_c),
            pltpu.make_async_copy(coarse_noise.at[0], noise_c, load_c),
            pltpu.make_async_copy(coarse_basis.at[0], basis_c, load_c),
        )

    wide = 2 * LANES
    chunks = z.fine_slots // wide
    fine_limit = z.fine_slots - me * z.fine
    medium_limit = z.medium_slots - me * z.medium

    def fine_loads(k):
        cols = pl.ds(k * wide if isinstance(k, int) else pl.multiple_of(k * wide, wide), wide)
        copies = [
            pltpu.make_async_copy(fine_state.at[:, :, cols], fine_next.at[:, :, cols], load_f.at[k]),
            pltpu.make_async_copy(fine_basis.at[:, :, cols], basis_f.at[:, :, cols], load_f.at[k]),
        ]
        for g in range(z.groups):
            rows = pl.ds(g * SUB, SUB)
            copies.append(
                pltpu.make_async_copy(fine_noise.at[:, rows, cols], noise_f.at[g, :, :, cols], load_f.at[k])
            )
        return copies

    def medium_loads(t):
        cols = pl.ds(t * LANES if isinstance(t, int) else pl.multiple_of(t * LANES, LANES), LANES)
        return (
            pltpu.make_async_copy(
                medium_state.at[:, :, :, cols], medium_next.at[t, :, pl.ds(0, z.medium)], load_m.at[t]
            ),
            pltpu.make_async_copy(medium_noise.at[:, :, :, cols], noise_m.at[t], load_m.at[t]),
            pltpu.make_async_copy(medium_basis.at[:, :, cols], basis_m.at[t], load_m.at[t]),
        )

    def start_fine(k):
        @pl.when(k * wide < fine_limit)
        def _():
            start(fine_loads(k))

    def start_medium(t):
        @pl.when(t * LANES < medium_limit)
        def _():
            start(medium_loads(t))

    def start(copies):
        for copy in copies:
            copy.start()

    @jax.named_scope("advance_coarse")
    def advance_coarse():
        with jax.named_scope("wait_coarse"):
            for copy in coarse_loads():
                copy.wait()
        mode = lax.broadcasted_iota(jnp.int32, (z.coarse, z.coarse_slots), 0)
        degree = lax.broadcasted_iota(jnp.int32, (z.coarse, z.coarse_slots), 1)
        inside = mode + degree < z.coarse_slots
        planes = []
        for c in range(2):
            new = decay[2] * coarse_next[c] + amp[2] * noise_c[c].astype(f32)
            new = jnp.where(inside, new, 0.0)
            coarse_next[c] = new
            planes.append(new)
        planes.append(basis_c[...].astype(f32))
        column_c = lax.broadcasted_iota(jnp.int32, (over, LANES), 1)
        for k, plane in enumerate(planes):
            rest = plane[:over, LANES:]
            last = plane[LANES:, : 2 * over]
            added = jnp.concatenate([jnp.zeros_like(last), last[:, :over], rest], axis=1)
            folded = jnp.where(column_c < 2 * over, plane[LANES - over : LANES, :LANES], added)
            for i in range(z.low):
                lo = i * owners - (LANES - over)
                rows = folded[lo : lo + owners] if lo >= 0 else plane[i * owners : (i + 1) * owners, :LANES]
                spread[(3 * i + k) * owners : (3 * i + k + 1) * owners, :] = rows
        for o in range(owners):
            first[o] = spread[pl.ds(o, z.first_rows, stride=owners), :].astype(bf16)

    def all_of(ref, count, k):
        some = ref.at[pl.ds(0, count)]
        return pltpu.make_async_remote_copy(
            some, some, sent.at[k], came.at[k], device_id={"scale": 1 - s, "lat": a}, device_id_type=MESH
        )

    def first_copy(o):
        return pltpu.make_async_remote_copy(
            first.at[o], landed.at[a], sent.at[0], came.at[0],
            device_id={"scale": s, "lat": quarter + o}, device_id_type=MESH,
        )

    def second_copy(p):
        return pltpu.make_async_remote_copy(
            second.at[p], got_coarse.at[mine], sent.at[1], came.at[1],
            device_id={"scale": s, "lat": p}, device_id_type=MESH,
        )

    def row_copy(p):
        return pltpu.make_async_remote_copy(
            send.at[p], got.at[me], sent.at[2], came.at[2],
            device_id=place(p), device_id_type=MESH,
        )

    lane = lax.broadcasted_iota(jnp.int32, (z.rows, 2 * LANES), 1) % SUB
    slack = fine_limit - lax.broadcasted_iota(jnp.int32, (SUB, wide), 0)
    slack = slack - lax.broadcasted_iota(jnp.int32, (SUB, wide), 1)

    @jax.named_scope("fine_chunk")
    def fine_chunk(k, _):
        for copy in fine_loads(k):
            copy.wait()
        cols = pl.ds(pl.multiple_of(k * wide, wide), wide)
        for g in range(z.groups):
            rows = slice(g * SUB, (g + 1) * SUB)
            keep = slack > g * SUB + k * wide
            for i in range(z.pairs // 2):
                two = slice(2 * i, 2 * i + 2)
                new = decay[0] * fine_next[two, rows, cols] + amp[0] * noise_f[g, two, :, cols].astype(f32)
                new = jnp.where(keep[None], new, 0.0)
                fine_next[two, rows, cols] = new
                half[g, 2 * SUB * i : 2 * SUB * (i + 1), :] = new.reshape(2 * SUB, wide).astype(bf16)
            basis = basis_f[rows, :, cols].reshape(SUB * z.rows, wide)
            all_pairs = lax.dot_general(basis, half[g], (((1,), (1,)), ((), ())), preferred_element_type=f32)
            total = all_pairs[: z.rows]
            for q in range(1, SUB):
                total = jnp.where(lane == q, all_pairs[q * z.rows : (q + 1) * z.rows], total)
            picked[g * z.rows : (g + 1) * z.rows, :] += total
        return 0

    target = lax.broadcasted_iota(jnp.int32, (2 * LANES, 2 * LANES), 1)
    wanted = (target % z.members) * (2 * SUB) + (target // z.members % 2) * SUB
    wanted = wanted + target // LANES * 4 + target // z.pairs % 4
    order = (lax.broadcasted_iota(jnp.int32, (2 * LANES, 2 * LANES), 0) == wanted).astype(f32).astype(bf16)
    @jax.named_scope("put_fine")
    def put_fine(g0, g1):
        moved = jnp.dot(picked[g0 * z.rows : g1 * z.rows, :].astype(bf16), order, preferred_element_type=f32)
        for g in range(g0, g1):
            for q in range(2):
                rows_f[pl.ds(2 * g + q, z.rows, stride=stride), :] = moved[
                    (g - g0) * z.rows : (g - g0 + 1) * z.rows, q * LANES : (q + 1) * LANES
                ]

    line = lax.broadcasted_iota(jnp.int32, (SUB, LANES), 0)
    column = lax.broadcasted_iota(jnp.int32, (SUB, LANES), 1)

    def weight(row, index):
        at_zero = (line == row) & (column < z.pairs) & (index == 0)
        return jnp.where(at_zero, 0.5, 1.0).astype(f32)

    @jax.named_scope("ship")
    def ship():
        scale_row = jnp.concatenate([weight(0, me), weight(fine_quads - SUB, me)], axis=0)
        for r in range(z.rows):
            rows = rows_f[r * stride : r * stride + 2 * SUB, :]
            send[r] = (rows.astype(bf16).astype(f32) * scale_row).astype(bf16)
        for i in range(1, lat):
            row_copy(s * lat + (a + i) % lat).start()
        pl.semaphore_wait(twin, 1)
        for i in range(lat):
            row_copy((1 - s) * lat + (a + i) % lat).start()
        got[me] = send[me]

    @jax.named_scope("send_first")
    def send_first():
        for i in range(owners):
            o = (a + i) % owners

            @pl.when(o + quarter != a)
            def _():
                first_copy(o).start()

        @pl.when(owner)
        def _():
            landed[a] = first[mine]

    flat_next = medium_next.reshape(mid_tiles * z.pairs * z.medium_room, LANES)
    flat_noise = noise_m.reshape(mid_tiles * z.pairs * z.medium, LANES)
    span, leap = 2 * z.medium, 2 * z.medium_room
    room = medium_limit - lax.broadcasted_iota(jnp.int32, (span, LANES), 0) // 2
    room = room - lax.broadcasted_iota(jnp.int32, (span, LANES), 1)
    lane4 = lax.broadcasted_iota(jnp.int32, (z.rows, LANES), 1) // z.pairs

    @jax.named_scope("medium_chunk")
    def medium_chunk(t, _):
        for copy in medium_loads(t):
            copy.wait()
        keep = room > t * LANES
        top = t * z.members * leap
        for e in range(z.members):
            at = pl.ds(pl.multiple_of(top + e * leap, 2), span)
            noise_at = pl.ds(pl.multiple_of((t * z.members + e) * span, SUB), span)
            new = decay[1] * flat_next[at, :] + amp[1] * flat_noise[noise_at, :].astype(f32)
            flat_next[at, :] = jnp.where(keep, new, 0.0)
        for q in range(medium_quads):
            for b in range(4):
                for c in range(2):
                    new = flat_next[pl.ds(top + 2 * (4 * q + b) + c, z.members, stride=leap), :]
                    at = q * LANES + b * z.pairs + c * z.members
                    half_m[at : at + z.members, :] = new.astype(bf16)
            basis = basis_m[t, 4 * q : 4 * q + 4].reshape(4 * z.rows, LANES)
            all_pairs = lax.dot_general(
                basis, half_m[q * LANES : (q + 1) * LANES, :], (((1,), (1,)), ((), ())), preferred_element_type=f32
            )
            total = all_pairs[: z.rows]
            for b in range(1, 4):
                total = jnp.where(lane4 == b, all_pairs[b * z.rows : (b + 1) * z.rows], total)
            picked_m[q * z.rows : (q + 1) * z.rows, :] += total
        return 0

    @jax.named_scope("put_medium")
    def put_medium():
        for q in range(medium_quads):
            rows_f[pl.ds(fine_quads + q, z.rows, stride=stride), :] = picked_m[q * z.rows : (q + 1) * z.rows, :]
        for spare in range(fine_quads + medium_quads, 2 * SUB):
            rows_f[pl.ds(spare, z.rows, stride=stride), :] = jnp.zeros((z.rows, LANES), f32)

    @jax.named_scope("fill_zeros")
    def fill_zeros():
        def fine_fill(k, _):
            cols = pl.ds(pl.multiple_of(k * wide, wide), wide)

            def pair_fill(i, _):
                fine_next[pl.ds(2 * i, 2), :, cols] = jnp.zeros((2, z.fine, wide), f32)
                return 0

            return lax.fori_loop(0, z.pairs // 2, pair_fill, 0)

        lax.fori_loop((fine_limit + wide - 1) // wide, chunks, fine_fill, 0)

        def medium_fill(t, _):
            def member_fill(e, _):
                at = pl.ds(pl.multiple_of((t * z.members + e) * leap, 2), span)
                flat_next[at, :] = jnp.zeros((span, LANES), f32)
                return 0

            return lax.fori_loop(0, z.members, member_fill, 0)

        lax.fori_loop((medium_limit + LANES - 1) // LANES, mid_tiles, medium_fill, 0)

    @jax.named_scope("wait_first")
    def wait_first():
        all_of(landed, lat - 1, 0).wait_recv()

    @jax.named_scope("coarse_rows")
    def coarse_rows():
        jump = z.first_rows + SUB
        for p in range(lat):
            landed_f[p * jump : p * jump + z.first_rows, :] = landed[p].astype(f32)
        lane = lax.broadcasted_iota(jnp.int32, (lat, LANES), 1)
        low, extra = z.low, over // owners
        plain = low - extra
        for i in range(low):
            for c in range(2):
                values = landed_f[pl.ds(3 * i + c, lat, stride=jump), :]
                right_c[i * z.pairs + c * z.members : i * z.pairs + (c + 1) * z.members, :] = values.astype(bf16)
            values = landed_f[pl.ds(3 * i + 2, lat, stride=jump), :]
            if i >= plain:
                j = i - plain
                for at, lo, hi in ((i, 0, 2), (i + extra, 2, 3), (z.piece + j, 3, 4)):
                    some = jnp.where((lane >= lo * over) & (lane < hi * over), values, 0.0)
                    left_c[at * lat : (at + 1) * lat, :] = some.astype(bf16)
            else:
                left_c[i * lat : (i + 1) * lat, :] = values.astype(bf16)
        all_pairs = lax.dot_general(
            left_c[...], right_c[...], (((1,), (1,)), ((), ())), preferred_element_type=f32
        )
        block = lane // z.pairs

        def tile(i, j):
            return all_pairs[i * lat : (i + 1) * lat, j * LANES : (j + 1) * LANES]

        for j in range(SUB):
            row = jnp.zeros((lat, LANES), f32)
            for t in range(4):
                i = 4 * j + t
                if i < z.piece:
                    value = tile(i, min(i, low - 1) // 4)
                    if i < extra:
                        value = value + tile(z.piece + i, (low - 1) // 4)
                    row = jnp.where(block == t, value, row)
            spread[pl.ds(j, lat, stride=pitch), :] = row
        scale_row = weight(0, mine)
        for p in range(lat):
            rows = spread[p * pitch : p * pitch + SUB, :].astype(bf16).astype(f32)
            second[p] = (rows * scale_row).astype(bf16)
        for i in range(1, lat):
            second_copy((a + i) % lat).start()
        got_coarse[mine] = second[a]

    line_t = lax.broadcasted_iota(jnp.int32, (SUB, z.wrap), 0)
    left_over = fine_quads - SUB

    def twice(index):
        cos, sin = turns(SUB, z.wrap, z.wrap, index)
        return 2.0 * cos, 2.0 * sin

    def turned(base, cos, sin):
        return base[0] * cos - base[1] * sin, base[0] * sin + base[1] * cos

    def keep_rows(at, upper, lower):
        for part in range(2):
            both = jnp.concatenate([upper[part], lower[part]], axis=0).astype(bf16)
            for t in range(z.wrap // LANES):
                lo = (2 * t + part) * LANES
                table[at, lo : lo + LANES] = both[:, t * LANES : (t + 1) * LANES]

    @jax.named_scope("start_table")
    def start_table():
        count = 2 * n
        step = medium_quads * lax.broadcasted_iota(jnp.int32, (count, z.wrap), 0)
        wave_cos[...], wave_sin[...] = turns(count, z.wrap, z.wrap, step)

    def wave(u):
        return wave_cos[pl.ds(u, 1), :], wave_sin[pl.ds(u, 1), :]

    @jax.named_scope("fill_table")
    def fill_table(lo, hi):
        base = twice(line_t)
        mixed = twice(jnp.where(line_t < left_over, SUB + line_t, line_t - left_over))

        def fill_rows(p, _):
            cos, sin = wave(2 * p)
            upper = turned(base, cos, sin)
            low_cos, low_sin = wave(p)
            cos = jnp.where(line_t < left_over, cos, low_cos)
            sin = jnp.where(line_t < left_over, sin, low_sin)
            at = pl.multiple_of(2 * SUB * p, 2 * SUB)
            keep_rows(pl.ds(at, 2 * SUB), upper, turned(mixed, cos, sin))
            return 0

        lax.fori_loop(lo, hi, fill_rows, 0, unroll=2)

    @jax.named_scope("end_table")
    def end_table():
        base = twice(owners * line_t)
        at = 2 * SUB * n
        tiles = []
        for u in range(owners // 4):
            for t in range(4):
                cos, sin = turns(1, z.wrap, z.wrap, u + owners // 4 * t)
                tiles.append(turned(base, cos, sin))
        for q in range(0, len(tiles), 2):
            keep_rows(slice(at + q * SUB, at + (q + 2) * SUB), tiles[q], tiles[q + 1])

    @jax.named_scope("collect")
    def collect():
        with jax.named_scope("rows_in"):
            all_of(got, n - 1, 2).wait()

        @pl.when(owner)
        def _():
            all_of(first, owners - 1, 0).wait_send()
            all_of(second, lat - 1, 1).wait_send()
            all_of(got_coarse, owners - 1, 1).wait_recv()

        @pl.when(jnp.logical_not(owner))
        def _():
            all_of(first, owners, 0).wait_send()
            all_of(got_coarse, owners, 1).wait_recv()

    @jax.named_scope("meet")
    def meet():
        pl.semaphore_wait(barrier, lat)
        pl.semaphore_signal(twin, inc=1, device_id={"scale": 1 - s, "lat": a}, device_id_type=MESH)

    fine_count = (fine_limit + wide - 1) // wide
    half_way = jnp.minimum(fine_count, 3)
    early = jnp.where(me < 2, half_way, jnp.where(me < SUB, 1, 0))
    many = fine_count > 3
    start(coarse_loads())
    greet()

    @pl.when(many)
    def _():
        start(fine_loads(0))

    start_table()

    @pl.when(jnp.logical_not(many))
    def _():
        start(fine_loads(0))

    start_fine(1)
    picked[...] = jnp.zeros_like(picked)
    picked_m[...] = jnp.zeros_like(picked_m)
    advance_coarse()
    start_fine(2)
    for t in range(mid_tiles):
        start_medium(t)
    for k in range(3, chunks):
        start_fine(k)
    lax.fori_loop(0, early, fine_chunk, 0)
    meet()
    send_first()
    lax.fori_loop(early, half_way, fine_chunk, 0)
    lax.fori_loop(0, (medium_limit + LANES - 1) // LANES, medium_chunk, 0)
    lax.fori_loop(half_way, fine_count, fine_chunk, 0)
    put_fine(0, z.groups)
    put_medium()

    ship()

    @pl.when(owner)
    def _():
        wait_first()
        coarse_rows()

    fill_table(0, n)
    end_table()
    fill_zeros()
    collect()


def grid_kernel(
    z, fine_in, medium_in, coarse_in, got, got_coarse, table, fine_out, medium_out, coarse_out, out, turned, sems
):
    copies = [
        pltpu.make_async_copy(fine_in, fine_out, sems.at[0]),
        pltpu.make_async_copy(coarse_in, coarse_out.at[0], sems.at[1]),
    ]
    for t in range(medium_in.shape[0]):
        cols = pl.ds(t * LANES, LANES)
        copies.append(pltpu.make_async_copy(medium_in.at[t, :, pl.ds(0, z.medium)], medium_out.at[:, :, :, cols], sems.at[2 + t]))
    for copy in copies:
        copy.start()
    with jax.named_scope("turn_rows"):
        turn_rows(z, got, got_coarse, turned)
    with jax.named_scope("sum_longitudes"):
        sum_longitudes(z, turned, table, out)
    with jax.named_scope("wait_writes"):
        for copy in copies:
            copy.wait()


def turn_rows(z, got, got_coarse, turned):
    many = 2 * z.n * SUB
    turned[:, :many] = got[...].reshape(many, LANES).astype(jnp.float32).T.astype(jnp.bfloat16)
    block = lax.broadcasted_iota(jnp.int32, (SUB, LANES), 1) // z.pairs
    few = []
    for u in range(z.owners // 4):
        for t in range(4):
            rows = jnp.zeros((SUB, LANES), jnp.float32)
            for b in range(4):
                some = got_coarse[4 * u + b].astype(jnp.float32)
                if b != t:
                    some = pltpu.roll(some, (b - t) % 4 * z.pairs, axis=1)
                rows = jnp.where(block == b, some, rows)
            few.append(rows)
    few = jnp.concatenate(few, axis=0)
    turned[:, many:] = few.T.astype(jnp.bfloat16)


def sum_longitudes(z, turned, table, out):
    e, tiles = z.members, z.wrap // LANES
    for t in range(tiles):
        both = jnp.dot(turned[...], table[:, 2 * t * LANES : 2 * (t + 1) * LANES], preferred_element_type=jnp.float32)
        waves = []
        for b in range(4):
            at = 2 * b * e
            cos_r, sin_r = both[at : at + e, :LANES], both[at : at + e, LANES:]
            cos_i, sin_i = both[at + e : at + 2 * e, :LANES], both[at + e : at + 2 * e, LANES:]
            re, im = cos_r - sin_i, sin_r + cos_i
            if b:
                angle = (lax.broadcasted_iota(jnp.int32, (1, LANES), 1) + t * LANES).astype(jnp.float32)
                angle = angle * (2.0 * math.pi * b / NLON)
                cos, sin = jnp.cos(angle), jnp.sin(angle)
                re, im = re * cos - im * sin, re * sin + im * cos
            waves.append((re, im))
        for h in range(4):
            total = None
            for b in range(4):
                re, im = waves[b]
                term = (re, -im, -re, im)[b * h % 4]
                total = term if total is None else total + term
            out[pl.ds(h * tiles + t, e, stride=4 * tiles), :] = jnp.tanh(total)


def fast_body(
    z,
    fine_state,
    fine_noise,
    medium_state,
    medium_noise,
    coarse_state,
    coarse_noise,
    decay,
    amplitude,
    fine_basis,
    medium_basis,
    coarse_basis,
):
    f32, bf16, dma = jnp.float32, jnp.bfloat16, pltpu.SemaphoreType.DMA
    e, n, lat, rows = z.members, z.n, z.lat, z.rows
    tiles = z.medium_slots // LANES
    owners = z.owners
    table_rows = 2 * n * SUB + owners * SUB
    operands = (
        decay,
        amplitude,
        fine_state.reshape(z.pairs, z.fine, z.fine_slots),
        fine_noise.reshape(z.pairs, z.fine, z.fine_slots),
        fine_basis,
        medium_state.transpose(0, 2, 1, 3),
        medium_noise.transpose(0, 2, 1, 3),
        medium_basis,
        coarse_state,
        coarse_noise,
        coarse_basis,
    )
    operands = tuple(pltpu.with_memory_space_constraint(x, pltpu.HBM) for x in operands)
    vmem = pl.BlockSpec(memory_space=pltpu.VMEM)
    hbm = pl.BlockSpec(memory_space=pltpu.HBM)
    between = (
        pltpu.VMEM((z.pairs, z.fine, z.fine_slots), f32),
        pltpu.VMEM((tiles, e, z.medium_room, 2, LANES), f32),
        pltpu.VMEM((2, z.coarse, z.coarse_slots), f32),
        pltpu.VMEM((n, 2 * SUB, LANES), bf16),
        pltpu.VMEM((owners, SUB, LANES), bf16),
        pltpu.VMEM((table_rows, 2 * z.wrap), bf16),
    )
    held = pl.pallas_call(
        functools.partial(spread_kernel, z),
        out_shape=between,
        in_specs=[hbm] * 11,
        out_specs=(vmem,) * 6,
        scratch_shapes=[
            pltpu.VMEM((z.groups, z.pairs, SUB, z.fine_slots), bf16),
            pltpu.VMEM((z.fine, rows, z.fine_slots), bf16),
            pltpu.VMEM((z.groups, SUB * z.pairs, 2 * LANES), bf16),
            pltpu.VMEM((z.groups * rows, 2 * LANES), f32),
            pltpu.VMEM((tiles, e, z.medium, 2, LANES), bf16),
            pltpu.VMEM((tiles, z.medium, rows, LANES), bf16),
            pltpu.VMEM((z.medium * z.pairs, LANES), bf16),
            pltpu.VMEM((z.medium // 4 * rows, LANES), f32),
            pltpu.VMEM((rows * 3 * SUB, LANES), f32),
            pltpu.VMEM((n, 2 * SUB, LANES), bf16),
            pltpu.VMEM((2, z.coarse, z.coarse_slots), bf16),
            pltpu.VMEM((z.coarse, z.coarse_slots), bf16),
            pltpu.VMEM((max(z.first_rows * owners, lat * 3 * SUB), LANES), f32),
            pltpu.VMEM((owners, z.first_rows, LANES), bf16),
            pltpu.VMEM((lat, z.first_rows, LANES), bf16),
            pltpu.VMEM((lat * (z.first_rows + SUB), LANES), f32),
            pltpu.VMEM(((2 * z.piece - z.low) * lat, LANES), bf16),
            pltpu.VMEM((z.low * z.pairs, LANES), bf16),
            pltpu.VMEM((lat, SUB, LANES), bf16),
            pltpu.VMEM((2 * n, z.wrap), f32),
            pltpu.VMEM((2 * n, z.wrap), f32),
            pltpu.SMEM((3,), f32),
            pltpu.SMEM((3,), f32),
            dma((z.fine_slots // (2 * LANES),)),
            dma((tiles,)),
            dma,
            dma((3,)),
            dma((3,)),
            pltpu.SemaphoreType.REGULAR,
        ],
        compiler_params=pltpu.CompilerParams(
            collective_id=0, has_side_effects=True, vmem_limit_bytes=32 * 1024 * 1024
        ),
    )(*operands)
    fine_next, medium_next, coarse_next, pattern = pl.pallas_call(
        functools.partial(grid_kernel, z),
        out_shape=(
            jax.ShapeDtypeStruct((z.pairs, z.fine, z.fine_slots), f32),
            jax.ShapeDtypeStruct((e, z.medium, 2, z.medium_slots), f32),
            jax.ShapeDtypeStruct(coarse_state.shape, f32),
            jax.ShapeDtypeStruct((e * NLON // LANES, LANES), f32),
        ),
        in_specs=[vmem] * 6,
        out_specs=(hbm, hbm, hbm, vmem),
        scratch_shapes=[pltpu.VMEM((LANES, table_rows), bf16), dma((2 + tiles,))],
        compiler_params=pltpu.CompilerParams(vmem_limit_bytes=32 * 1024 * 1024),
    )(*held)
    return (
        fine_next.reshape(fine_state.shape),
        medium_next.transpose(0, 2, 1, 3),
        coarse_next,
        pattern.reshape(e, 1, NLON),
    )


def body(*arrays):
    fine_state, medium_state, coarse_state = arrays[0], arrays[2], arrays[4]
    scale, lat = lax.axis_size("scale"), lax.axis_size("lat")
    z = Sizes(fine_state, medium_state, coarse_state, arrays[8], arrays[10], scale, lat)
    return fast_body(z, *arrays) if z.fits() else general_body(*arrays)


def solution(mesh):
    return jax.shard_map(
        body,
        mesh=mesh,
        in_specs=(
            P(None, None, ("scale", "lat"), None),
            P(None, None, ("scale", "lat"), None),
            P(None, None, ("scale", "lat"), None),
            P(None, None, ("scale", "lat"), None),
            P("lat", None, None, None),
            P("lat", None, None, None),
            P(),
            P(),
            P(("scale", "lat"), None, None),
            P(("scale", "lat"), None, None),
            P(("scale", "lat"), None, None),
        ),
        out_specs=(
            P(None, None, ("scale", "lat"), None),
            P(None, None, ("scale", "lat"), None),
            P("lat", None, None, None),
            P(None, ("scale", "lat"), None),
        ),
        check_vma=False,
    )
```

```python
import functools
import math

import jax
import jax.numpy as jnp
import numpy as np
from jax import lax
from jax.experimental import pallas as pl
from jax.experimental.pallas import tpu as pltpu
from jax.sharding import PartitionSpec as P

NLON = 2560
LANES = 128
FOLD = NLON // LANES


def advance(state, noise, decay_rate, amp_rate, offset):
    slots = state.shape[3]
    mode_ids = offset + jnp.arange(state.shape[2], dtype=jnp.int32)
    degree_ids = jnp.arange(slots, dtype=jnp.int32)
    inside = mode_ids[:, None] + degree_ids[None, :] < slots
    updated = decay_rate * state + amp_rate * noise.astype(jnp.float32)
    return jnp.where(inside, updated, jnp.zeros_like(updated))


def phase_rows(block, devices):
    return max((p * block % FOLD + block - 1) // FOLD + 1 for p in range(devices))


def phase_blocks(fourier, place, devices, modes=None):
    rows, parts, block, members = fourier.shape
    high = phase_rows(block, devices)
    if block % FOLD:
        start = (place * block % FOLD).astype(jnp.int32)
        room = jnp.zeros((rows, parts, high * FOLD, members), fourier.dtype)
        zero = jnp.zeros((), jnp.int32)
        fourier = lax.dynamic_update_slice(room, fourier, (zero, zero, start, zero))
    return fourier.reshape(rows, parts * high, FOLD * members)


def received_rows(blocks, devices, width):
    source = np.arange(devices, dtype=np.int32)
    cols, parts = [], []
    for block in blocks:
        for part in range(2):
            for j in range(phase_rows(block, devices)):
                cols.append(source * block // FOLD + j)
                parts.append(part)
    while len(cols) < width:
        cols.append(source * 0)
        parts.append(0)
    high = np.stack(cols, axis=1).reshape(-1, 1)
    part = np.tile(np.array(parts, np.int32), devices)[:, None]
    return np.concatenate([high, part], axis=1).astype(np.int32)


def table_kernel(rows_ref, table_ref):
    count = rows_ref.shape[0]
    high, part = rows_ref[:, 0:1], rows_ref[:, 1:2]
    lon = lax.broadcasted_iota(jnp.int32, (count, LANES), 1)
    turns = (high * lon + part * (LANES // 4)) % LANES
    angle = turns.astype(jnp.float32) * (2.0 * math.pi / LANES)
    re, im = 2.0 * jnp.cos(angle), 2.0 * jnp.sin(angle)
    first = jnp.where(high == 0, 0.5, 1.0).astype(jnp.float32)
    shape = (-(-FOLD // 8) * 8, LANES)
    low = lax.broadcasted_iota(jnp.int32, shape, 0) * lax.broadcasted_iota(jnp.int32, shape, 1)
    low = low.astype(jnp.float32) * (2.0 * math.pi / NLON)
    cos, sin = jnp.cos(low), jnp.sin(low)
    for q in range(FOLD):
        cl, sl = cos[q : q + 1], sin[q : q + 1]
        real, imag = re * cl - im * sl, im * cl + re * sl
        if q == 0:
            real, imag = real * first, imag * first
        table_ref[q, :, :LANES] = real.astype(jnp.bfloat16)
        table_ref[q, :, LANES:] = imag.astype(jnp.bfloat16)


def longitude_kernel(members, got_ref, table_ref, out_ref):
    own = got_ref.shape[1]
    for i in range(own):
        spread = got_ref[:, i].astype(jnp.float32)
        spread = spread.reshape(spread.shape[0] * spread.shape[1], spread.shape[2])
        lanes = -spread.shape[1] % LANES
        if lanes:
            spread = jnp.concatenate(
                [spread, jnp.zeros((spread.shape[0], lanes), jnp.float32)], axis=1
            )
        turned = spread.T.astype(jnp.bfloat16)
        totals = [None] * FOLD
        for q in range(FOLD):
            part = jnp.dot(
                turned[q * members : (q + 1) * members],
                table_ref[q],
                preferred_element_type=jnp.float32,
            )
            real, imag = part[:, :LANES], part[:, LANES:]
            for h in range(FOLD):
                turn = 2.0 * math.pi * (q * h % FOLD) / FOLD
                term = math.cos(turn) * real - math.sin(turn) * imag
                totals[h] = term if q == 0 else totals[h] + term
        for h in range(FOLD):
            out_ref[:, i, h * LANES : (h + 1) * LANES] = jnp.tanh(totals[h])


def coarse_kernel(
    part_modes, decay_ref, amp_ref, state_ref, noise_ref, basis_ref, next_ref, mixed_ref, fine_ref, medium_ref
):
    held, parts, modes, slots = state_ref.shape
    for scale, rate_ref in ((0, fine_ref), (1, medium_ref)):
        rate_ref[0:1] = jnp.full((1, rate_ref.shape[1]), decay_ref[scale], jnp.float32)
        rate_ref[1:2] = jnp.full((1, rate_ref.shape[1]), amp_ref[scale], jnp.float32)
    mode_ids = lax.broadcasted_iota(jnp.int32, (modes, slots), 0)
    degree_ids = lax.broadcasted_iota(jnp.int32, (modes, slots), 1)
    inside = mode_ids + degree_ids < slots
    planes = []
    for e in range(held):
        for c in range(parts):
            new = decay_ref[2] * state_ref[e, c] + amp_ref[2] * noise_ref[e, c].astype(jnp.float32)
            new = jnp.where(inside, new, 0.0)
            next_ref[e, c] = new
            planes.append(new)
    for r in range(basis_ref.shape[0]):
        planes.append(basis_ref[r].astype(jnp.float32))
    empty = jnp.zeros((part_modes, slots), jnp.float32)
    for d in range(mixed_ref.shape[0]):
        pieces = []
        for plane in planes:
            piece = plane[d * part_modes : min((d + 1) * part_modes, modes)]
            missing = part_modes - piece.shape[0]
            if missing == part_modes:
                piece = empty
            elif missing:
                piece = jnp.concatenate([piece, empty[:missing]], axis=0)
            pieces.append(piece)
        mixed_ref[d] = jnp.concatenate(pieces, axis=0).astype(jnp.bfloat16)


def general_body(
    fine_state,
    fine_noise,
    medium_state,
    medium_noise,
    coarse_state,
    coarse_noise,
    decay,
    amplitude,
    fine_basis,
    medium_basis,
    coarse_basis,
):
    devices = lax.axis_size("scale") * lax.axis_size("lat")
    lat = lax.axis_size("lat")
    held, _, modes, slots = coarse_state.shape
    own = coarse_basis.shape[0]
    part_modes = -(-modes // devices)
    vmem = pl.BlockSpec(memory_space=pltpu.VMEM)
    smem = pl.BlockSpec(memory_space=pltpu.SMEM)
    coarse_next, mixed, fine_rates, medium_rates = pl.pallas_call(
        functools.partial(coarse_kernel, part_modes),
        out_shape=(
            jax.ShapeDtypeStruct(coarse_state.shape, jnp.float32),
            jax.ShapeDtypeStruct((devices, (2 * held + own) * part_modes, slots), jnp.bfloat16),
            jax.ShapeDtypeStruct((2, fine_state.shape[3]), jnp.float32),
            jax.ShapeDtypeStruct((2, medium_state.shape[3]), jnp.float32),
        ),
        in_specs=[smem, smem, vmem, vmem, vmem],
        out_specs=(vmem,) * 4,
    )(decay, amplitude, coarse_state, coarse_noise, coarse_basis)
    mixed = lax.all_to_all(mixed, ("scale", "lat"), split_axis=0, concat_axis=0, tiled=True)
    mixed = mixed.reshape(devices, 2 * held + own, part_modes, slots)
    coarse_half = mixed[:lat, : 2 * held].reshape(lat * held, 2, part_modes, slots)
    coarse_rows = mixed[:, 2 * held :].reshape(devices * own, part_modes, slots)
    place = lax.axis_index(("scale", "lat"))
    fine_next = advance(fine_state, fine_noise, fine_rates[0], fine_rates[1], place * fine_state.shape[2])
    medium_next = advance(
        medium_state, medium_noise, medium_rates[0], medium_rates[1], place * medium_state.shape[2]
    )
    fourier = []
    for half, basis, form in (
        (fine_next.astype(jnp.bfloat16), fine_basis, "ecmk,mrk->rcme"),
        (medium_next.astype(jnp.bfloat16), medium_basis, "ecmk,mrk->rcme"),
        (coarse_half, coarse_rows, "ecmk,rmk->rcme"),
    ):
        fourier.append(
            jnp.einsum(form, half, basis, preferred_element_type=jnp.float32).astype(jnp.bfloat16)
        )
    members = coarse_half.shape[0]
    blocks = [x.shape[2] for x in fourier]
    both = jnp.concatenate([phase_blocks(x, place, devices) for x in fourier], axis=1)
    width = -(-both.shape[1] // 8) * 8
    both = jnp.pad(both, ((0, 0), (0, width - both.shape[1]), (0, 0)))
    received = received_rows(blocks, devices, width)
    table = pl.pallas_call(
        table_kernel,
        out_shape=jax.ShapeDtypeStruct((FOLD, devices * width, 2 * LANES), jnp.bfloat16),
        in_specs=[vmem],
        out_specs=vmem,
        cost_estimate=pl.CostEstimate(
            flops=30 * FOLD * devices * width * LANES,
            bytes_accessed=8 * FOLD * devices * width * LANES,
            transcendentals=4 * devices * width * LANES,
        ),
    )(jnp.asarray(received))
    got = lax.all_to_all(both, ("scale", "lat"), split_axis=0, concat_axis=0, tiled=True)
    got = got.reshape(devices, own, width, FOLD * members)
    pattern = pl.pallas_call(
        functools.partial(longitude_kernel, members),
        out_shape=jax.ShapeDtypeStruct((members, own, NLON), jnp.float32),
        in_specs=[vmem, vmem],
        out_specs=vmem,
    )(got, table)
    return (fine_next, medium_next, coarse_next, pattern)


MESH = pl.DeviceIdType.MESH
SUB = 8


class Sizes:
    def __init__(self, fine_state, medium_state, coarse_state, fine_basis, coarse_basis, scale, lat):
        self.scale, self.lat, self.n = scale, lat, scale * lat
        _, self.parts, self.fine, self.fine_slots = fine_state.shape
        self.members = fine_state.shape[0]
        self.pairs = self.members * self.parts
        self.medium, self.medium_slots = medium_state.shape[2:]
        self.coarse, self.coarse_slots = coarse_state.shape[2:]
        self.held, self.own, self.rows = coarse_state.shape[0], coarse_basis.shape[0], fine_basis.shape[1]
        self.groups = self.fine // SUB
        self.quad = LANES // self.pairs
        self.medium_room = self.medium + 1
        self.quarter, self.owners = lat // 4, lat // 2
        self.piece = self.coarse // max(self.owners, 1)
        self.low = LANES // max(self.owners, 1)
        self.first_rows = -(-3 * self.low // SUB) * SUB
        self.wrap = NLON // max(self.quad, 1)

    def fits(self):
        if self.pairs * 4 != LANES or self.parts != 2 or self.held != 1 or self.own != 1:
            return False
        if self.rows != self.n or self.members != self.lat or self.members != 16:
            return False
        if self.fine_slots <= AHEAD * 2 * LANES or self.fine % SUB or self.medium % 4 or self.fine != 2 * self.medium:
            return False
        if self.fine_slots % (2 * LANES) or self.medium_slots % LANES or self.scale != 2:
            return False
        over = self.coarse_slots - LANES
        if self.coarse_slots != self.coarse or 4 * over != LANES or over % self.owners:
            return False
        if self.owners != SUB or self.coarse % self.owners or over // self.owners != 4 or self.low % 4 or self.piece > 4 * SUB:
            return False
        if self.n * self.fine > self.fine_slots or self.n * self.medium > self.medium_slots:
            return False
        high = self.fine // 4
        return SUB <= high and high - SUB + self.medium // 4 <= SUB and self.wrap % LANES == 0


def turns(count, columns, period, index):
    lon = lax.broadcasted_iota(jnp.int32, (count, columns), 1)
    angle = ((index * lon) % period).astype(jnp.float32) * (2.0 * math.pi / period)
    return jnp.cos(angle), jnp.sin(angle)


def spread_kernel(
    z,
    decay_in,
    amp_in,
    fine_state,
    fine_noise,
    fine_basis,
    medium_state,
    medium_noise,
    medium_basis,
    coarse_state,
    coarse_noise,
    coarse_basis,
    begun,
    fine_next,
    medium_next,
    coarse_next,
    got,
    got_coarse,
    table,
    noise_f,
    basis_f,
    half,
    picked,
    noise_m,
    basis_m,
    half_m,
    picked_m,
    rows_f,
    send,
    noise_c,
    basis_c,
    spread,
    first,
    landed,
    landed_f,
    left_c,
    right_c,
    second,
    wave_cos,
    wave_sin,
    decay,
    amp,
    load_f,
    load_m,
    load_c,
    sent,
    came,
    twin,
    here,
):
    n, lat = z.n, z.lat
    s, a = lax.axis_index("scale"), lax.axis_index("lat")
    me = s * lat + a
    f32, bf16 = jnp.float32, jnp.bfloat16
    mid_tiles = z.medium_slots // LANES
    fine_quads, medium_quads = z.fine // 4, z.medium // 4
    over = z.coarse_slots - LANES
    stride, pitch = 3 * SUB, 3 * SUB

    def place(p):
        return {"scale": p // lat, "lat": p % lat}

    barrier = pltpu.get_barrier_semaphore()

    quarter, owners = z.quarter, z.owners
    owner = (a >= quarter) & (a < quarter + owners)
    mine = jnp.where(owner, a - quarter, 0)

    step = jnp.where(a < lat // 2, -1, 1)

    def greet():
        @pl.when(owner)
        def _():
            for i in range(1, lat):
                near = {"scale": s, "lat": (a + i) % lat}
                pl.semaphore_signal(barrier, inc=1, device_id=near, device_id_type=MESH)

        pl.semaphore_signal(barrier, inc=1, device_id={"scale": 1 - s, "lat": a}, device_id_type=MESH)

    def coarse_loads():
        return (
            pltpu.make_async_copy(decay_in, decay, load_c),
            pltpu.make_async_copy(amp_in, amp, load_c),
            pltpu.make_async_copy(coarse_state.at[0], coarse_next, load_c),
            pltpu.make_async_copy(coarse_noise.at[0], noise_c, load_c),
            pltpu.make_async_copy(coarse_basis.at[0], basis_c, load_c),
        )

    wide = 2 * LANES
    chunks = z.fine_slots // wide
    fine_limit = z.fine_slots - me * z.fine
    medium_limit = z.medium_slots - me * z.medium

    def fine_loads(k):
        cols = pl.ds(k * wide if isinstance(k, int) else pl.multiple_of(k * wide, wide), wide)
        copies = [
            pltpu.make_async_copy(fine_state.at[:, :, cols], fine_next.at[:, :, cols], load_f.at[k]),
            pltpu.make_async_copy(fine_basis.at[:, :, cols], basis_f.at[:, :, cols], load_f.at[k]),
        ]
        for g in range(z.groups):
            rows = pl.ds(g * SUB, SUB)
            copies.append(
                pltpu.make_async_copy(fine_noise.at[:, rows, cols], noise_f.at[g, :, :, cols], load_f.at[k])
            )
        return copies

    def medium_loads(t):
        cols = pl.ds(t * LANES if isinstance(t, int) else pl.multiple_of(t * LANES, LANES), LANES)
        return (
            pltpu.make_async_copy(
                medium_state.at[:, :, :, cols], medium_next.at[t, :, pl.ds(0, z.medium)], load_m.at[t]
            ),
            pltpu.make_async_copy(medium_noise.at[:, :, :, cols], noise_m.at[t], load_m.at[t]),
            pltpu.make_async_copy(medium_basis.at[:, :, cols], basis_m.at[t], load_m.at[t]),
        )

    def start_fine(k):
        @pl.when(k * wide < fine_limit)
        def _():
            start(fine_loads(k))

    def start_medium(t):
        @pl.when(t * LANES < medium_limit)
        def _():
            start(medium_loads(t))

    def start(copies):
        for copy in copies:
            copy.start()

    @jax.named_scope("advance_coarse")
    def advance_coarse():
        with jax.named_scope("wait_coarse"):
            for copy in coarse_loads():
                copy.wait()
        mode = lax.broadcasted_iota(jnp.int32, (z.coarse, z.coarse_slots), 0)
        degree = lax.broadcasted_iota(jnp.int32, (z.coarse, z.coarse_slots), 1)
        inside = mode + degree < z.coarse_slots
        planes = []
        for c in range(2):
            new = decay[2] * coarse_next[c] + amp[2] * noise_c[c].astype(f32)
            new = jnp.where(inside, new, 0.0)
            coarse_next[c] = new
            planes.append(new)
        planes.append(basis_c[...].astype(f32))
        column_c = lax.broadcasted_iota(jnp.int32, (over, LANES), 1)
        for k, plane in enumerate(planes):
            rest = plane[:over, LANES:]
            last = plane[LANES:, : 2 * over]
            added = jnp.concatenate([jnp.zeros_like(last), last[:, :over], rest], axis=1)
            folded = jnp.where(column_c < 2 * over, plane[LANES - over : LANES, :LANES], added)
            for i in range(z.low):
                lo = i * owners - (LANES - over)
                rows = folded[lo : lo + owners] if lo >= 0 else plane[i * owners : (i + 1) * owners, :LANES]
                spread[(3 * i + k) * owners : (3 * i + k + 1) * owners, :] = rows
        for o in range(owners):
            first[o] = spread[pl.ds(o, z.first_rows, stride=owners), :].astype(bf16)

    def all_of(ref, count, k):
        some = ref.at[pl.ds(0, count)]
        return pltpu.make_async_remote_copy(
            some, some, sent.at[k], came.at[k], device_id={"scale": 1 - s, "lat": a}, device_id_type=MESH
        )

    def first_copy(o):
        return pltpu.make_async_remote_copy(
            first.at[o], landed.at[a], sent.at[0], came.at[0],
            device_id={"scale": s, "lat": quarter + o}, device_id_type=MESH,
        )

    def second_copy(p):
        return pltpu.make_async_remote_copy(
            second.at[p], got_coarse.at[mine], sent.at[1], came.at[1],
            device_id={"scale": s, "lat": p}, device_id_type=MESH,
        )

    def row_copy(p):
        return pltpu.make_async_remote_copy(
            send.at[p], got.at[me], sent.at[2], came.at[2],
            device_id=place(p), device_id_type=MESH,
        )

    lane = lax.broadcasted_iota(jnp.int32, (z.rows, 2 * LANES), 1) % SUB
    slack = fine_limit - lax.broadcasted_iota(jnp.int32, (SUB, wide), 0)
    slack = slack - lax.broadcasted_iota(jnp.int32, (SUB, wide), 1)

    @jax.named_scope("fine_chunk")
    def fine_chunk(k, _):
        for copy in fine_loads(k):
            copy.wait()
        cols = pl.ds(pl.multiple_of(k * wide, wide), wide)
        for g in range(z.groups):
            rows = slice(g * SUB, (g + 1) * SUB)
            keep = slack > g * SUB + k * wide
            for i in range(z.pairs // 2):
                two = slice(2 * i, 2 * i + 2)
                new = decay[0] * fine_next[two, rows, cols] + amp[0] * noise_f[g, two, :, cols].astype(f32)
                new = jnp.where(keep[None], new, 0.0)
                fine_next[two, rows, cols] = new
                half[g, 2 * SUB * i : 2 * SUB * (i + 1), :] = new.reshape(2 * SUB, wide).astype(bf16)
            basis = basis_f[rows, :, cols].reshape(SUB * z.rows, wide)
            all_pairs = lax.dot_general(basis, half[g], (((1,), (1,)), ((), ())), preferred_element_type=f32)
            total = all_pairs[: z.rows]
            for q in range(1, SUB):
                total = jnp.where(lane == q, all_pairs[q * z.rows : (q + 1) * z.rows], total)
            picked[g * z.rows : (g + 1) * z.rows, :] += total
        return 0

    target = lax.broadcasted_iota(jnp.int32, (2 * LANES, 2 * LANES), 1)
    wanted = (target % z.members) * (2 * SUB) + (target // z.members % 2) * SUB
    wanted = wanted + target // LANES * 4 + target // z.pairs % 4
    order = (lax.broadcasted_iota(jnp.int32, (2 * LANES, 2 * LANES), 0) == wanted).astype(f32).astype(bf16)
    @jax.named_scope("put_fine")
    def put_fine(g0, g1):
        moved = jnp.dot(picked[g0 * z.rows : g1 * z.rows, :].astype(bf16), order, preferred_element_type=f32)
        for g in range(g0, g1):
            for q in range(2):
                rows_f[pl.ds(2 * g + q, z.rows, stride=stride), :] = moved[
                    (g - g0) * z.rows : (g - g0 + 1) * z.rows, q * LANES : (q + 1) * LANES
                ]

    line = lax.broadcasted_iota(jnp.int32, (SUB, LANES), 0)
    column = lax.broadcasted_iota(jnp.int32, (SUB, LANES), 1)

    def weight(row, index):
        at_zero = (line == row) & (column < z.pairs) & (index == 0)
        return jnp.where(at_zero, 0.5, 1.0).astype(f32)

    @jax.named_scope("ship")
    def ship():
        scale_row = jnp.concatenate([weight(0, me), weight(fine_quads - SUB, me)], axis=0)
        for r in range(z.rows):
            rows = rows_f[r * stride : r * stride + 2 * SUB, :]
            send[r] = (rows.astype(bf16).astype(f32) * scale_row).astype(bf16)
        @pl.when(s == 1)
        def _():
            pl.semaphore_wait(twin, 1)
            for p in range(2):
                row_copy(p).start()

        for p in range(lat):

            @pl.when(a != p)
            def _():
                row_copy(s * lat + p).start()

        @pl.when(s == 0)
        def _():
            pl.semaphore_wait(twin, 1)
            for p in range(lat):
                row_copy(lat + p).start()

        @pl.when(s == 1)
        def _():
            for p in range(2, lat):
                row_copy(p).start()

        got[me] = send[me]

    @jax.named_scope("send_first")
    def send_first():
        turn = a
        for i in range(owners):
            o = (turn + i) % owners

            @pl.when(o + quarter != a)
            def _():
                first_copy(o).start()

        @pl.when(owner)
        def _():
            landed[a] = first[mine]

    flat_next = medium_next.reshape(mid_tiles * z.pairs * z.medium_room, LANES)
    flat_noise = noise_m.reshape(mid_tiles * z.pairs * z.medium, LANES)
    span, leap = 2 * z.medium, 2 * z.medium_room
    room = medium_limit - lax.broadcasted_iota(jnp.int32, (span, LANES), 0) // 2
    room = room - lax.broadcasted_iota(jnp.int32, (span, LANES), 1)
    lane4 = lax.broadcasted_iota(jnp.int32, (z.rows, LANES), 1) // z.pairs

    @jax.named_scope("medium_chunk")
    def medium_chunk(t, _):
        for copy in medium_loads(t):
            copy.wait()
        medium_work(t, 0)
        return 0

    @jax.named_scope("medium_pair")
    def medium_pair(i, _):
        for k in range(2):
            for copy in medium_loads(1 + 2 * i + k):
                copy.wait()
        for k in range(2):
            medium_work(1 + 2 * i + k, k)
        return 0

    def medium_work(t, slot):
        keep = room > t * LANES
        top = t * z.members * leap
        for e in range(z.members):
            at = pl.ds(pl.multiple_of(top + e * leap, 2), span)
            noise_at = pl.ds(pl.multiple_of((t * z.members + e) * span, SUB), span)
            new = decay[1] * flat_next[at, :] + amp[1] * flat_noise[noise_at, :].astype(f32)
            flat_next[at, :] = jnp.where(keep, new, 0.0)
        for q in range(medium_quads):
            for b in range(4):
                for c in range(2):
                    new = flat_next[pl.ds(top + 2 * (4 * q + b) + c, z.members, stride=leap), :]
                    at = q * LANES + b * z.pairs + c * z.members
                    half_m[slot, at : at + z.members, :] = new.astype(bf16)
            basis = basis_m[t, 4 * q : 4 * q + 4].reshape(4 * z.rows, LANES)
            all_pairs = lax.dot_general(
                basis, half_m[slot, q * LANES : (q + 1) * LANES, :], (((1,), (1,)), ((), ())), preferred_element_type=f32
            )
            total = all_pairs[: z.rows]
            for b in range(1, 4):
                total = jnp.where(lane4 == b, all_pairs[b * z.rows : (b + 1) * z.rows], total)
            picked_m[q * z.rows : (q + 1) * z.rows, :] += total

    @jax.named_scope("put_medium")
    def put_medium():
        for q in range(medium_quads):
            rows_f[pl.ds(fine_quads + q, z.rows, stride=stride), :] = picked_m[q * z.rows : (q + 1) * z.rows, :]
        for spare in range(fine_quads + medium_quads, 2 * SUB):
            rows_f[pl.ds(spare, z.rows, stride=stride), :] = jnp.zeros((z.rows, LANES), f32)

    @jax.named_scope("fill_zeros")
    def fill_zeros():
        def fine_fill(k, _):
            cols = pl.ds(pl.multiple_of(k * wide, wide), wide)

            def pair_fill(i, _):
                fine_next[pl.ds(2 * i, 2), :, cols] = jnp.zeros((2, z.fine, wide), f32)
                return 0

            return lax.fori_loop(0, z.pairs // 2, pair_fill, 0)

        lax.fori_loop((fine_limit + wide - 1) // wide, chunks, fine_fill, 0)

        def medium_fill(t, _):
            def member_fill(e, _):
                at = pl.ds(pl.multiple_of((t * z.members + e) * leap, 2), span)
                flat_next[at, :] = jnp.zeros((span, LANES), f32)
                return 0

            return lax.fori_loop(0, z.members, member_fill, 0)

        lax.fori_loop((medium_limit + LANES - 1) // LANES, mid_tiles, medium_fill, 0)

    @jax.named_scope("wait_first")
    def wait_first():
        all_of(landed, lat - 1, 0).wait_recv()

    @jax.named_scope("coarse_rows")
    def coarse_rows():
        jump = z.first_rows + SUB
        for p in range(lat):
            landed_f[p * jump : p * jump + z.first_rows, :] = landed[p].astype(f32)
        lane = lax.broadcasted_iota(jnp.int32, (lat, LANES), 1)
        low, extra = z.low, over // owners
        plain = low - extra
        for i in range(low):
            for c in range(2):
                values = landed_f[pl.ds(3 * i + c, lat, stride=jump), :]
                right_c[i * z.pairs + c * z.members : i * z.pairs + (c + 1) * z.members, :] = values.astype(bf16)
            values = landed_f[pl.ds(3 * i + 2, lat, stride=jump), :]
            if i >= plain:
                j = i - plain
                for at, lo, hi in ((i, 0, 2), (i + extra, 2, 3), (z.piece + j, 3, 4)):
                    some = jnp.where((lane >= lo * over) & (lane < hi * over), values, 0.0)
                    left_c[at * lat : (at + 1) * lat, :] = some.astype(bf16)
            else:
                left_c[i * lat : (i + 1) * lat, :] = values.astype(bf16)
        all_pairs = lax.dot_general(
            left_c[...], right_c[...], (((1,), (1,)), ((), ())), preferred_element_type=f32
        )
        block = lane // z.pairs

        def tile(i, j):
            return all_pairs[i * lat : (i + 1) * lat, j * LANES : (j + 1) * LANES]

        for j in range(SUB):
            row = jnp.zeros((lat, LANES), f32)
            for t in range(4):
                i = 4 * j + t
                if i < z.piece:
                    value = tile(i, min(i, low - 1) // 4)
                    if i < extra:
                        value = value + tile(z.piece + i, (low - 1) // 4)
                    row = jnp.where(block == t, value, row)
            spread[pl.ds(j, lat, stride=pitch), :] = row
        scale_row = weight(0, mine)
        for p in range(lat):
            rows = spread[p * pitch : p * pitch + SUB, :].astype(bf16).astype(f32)
            second[p] = (rows * scale_row).astype(bf16)
        for p in range(lat):

            @pl.when(a != p)
            def _():
                second_copy(p).start()

        got_coarse[mine] = second[a]

    line_t = lax.broadcasted_iota(jnp.int32, (SUB, z.wrap), 0)
    left_over = fine_quads - SUB

    def twice(index):
        cos, sin = turns(SUB, z.wrap, z.wrap, index)
        return 2.0 * cos, 2.0 * sin

    def turned(base, cos, sin):
        return base[0] * cos - base[1] * sin, base[0] * sin + base[1] * cos

    def keep_rows(at, upper, lower):
        for part in range(2):
            both = jnp.concatenate([upper[part], lower[part]], axis=0).astype(bf16)
            for t in range(z.wrap // LANES):
                lo = (2 * t + part) * LANES
                table[at, lo : lo + LANES] = both[:, t * LANES : (t + 1) * LANES]

    @jax.named_scope("start_table")
    def start_table():
        count = 2 * n
        step = medium_quads * lax.broadcasted_iota(jnp.int32, (count, z.wrap), 0)
        wave_cos[...], wave_sin[...] = turns(count, z.wrap, z.wrap, step)

    def wave(u):
        return wave_cos[pl.ds(u, 1), :], wave_sin[pl.ds(u, 1), :]

    @jax.named_scope("fill_table")
    def fill_table(lo, hi):
        base = twice(line_t)
        mixed = twice(jnp.where(line_t < left_over, SUB + line_t, line_t - left_over))

        def fill_rows(p, _):
            cos, sin = wave(2 * p)
            upper = turned(base, cos, sin)
            low_cos, low_sin = wave(p)
            cos = jnp.where(line_t < left_over, cos, low_cos)
            sin = jnp.where(line_t < left_over, sin, low_sin)
            at = pl.multiple_of(2 * SUB * p, 2 * SUB)
            keep_rows(pl.ds(at, 2 * SUB), upper, turned(mixed, cos, sin))
            return 0

        lax.fori_loop(lo, hi, fill_rows, 0, unroll=2)

    @jax.named_scope("end_table")
    def end_table():
        base = twice(owners * line_t)
        at = 2 * SUB * n
        tiles = []
        for u in range(owners // 4):
            for t in range(4):
                cos, sin = turns(1, z.wrap, z.wrap, u + owners // 4 * t)
                tiles.append(turned(base, cos, sin))
        for q in range(0, len(tiles), 2):
            keep_rows(slice(at + q * SUB, at + (q + 2) * SUB), tiles[q], tiles[q + 1])

    @jax.named_scope("collect")
    def collect():
        with jax.named_scope("rows_in"):
            all_of(got, n - 1, 2).wait()

        @pl.when(owner)
        def _():
            all_of(first, owners - 1, 0).wait_send()
            all_of(second, lat - 1, 1).wait_send()
            all_of(got_coarse, owners - 1, 1).wait_recv()

        @pl.when(jnp.logical_not(owner))
        def _():
            all_of(first, owners, 0).wait_send()
            all_of(got_coarse, owners, 1).wait_recv()

    @jax.named_scope("meet")
    def meet():
        @pl.when(owner)
        def _():
            pl.semaphore_wait(barrier, owners)

        @pl.when(jnp.logical_not(owner))
        def _():
            pl.semaphore_wait(barrier, owners + 1)
            for i in range(owners):
                to = {"scale": s, "lat": quarter + (a + i) % owners}
                pl.semaphore_signal(here, inc=1, device_id=to, device_id_type=MESH)

    def tell_twin():
        pl.semaphore_signal(twin, inc=1, device_id={"scale": 1 - s, "lat": a}, device_id_type=MESH)

    @jax.named_scope("hear")
    def hear():
        @pl.when(owner)
        def _():
            pl.semaphore_wait(here, lat - owners)
            other = jnp.where(mine < quarter, mine, mine + owners)
            pl.semaphore_signal(here, inc=1, device_id={"scale": s, "lat": other}, device_id_type=MESH)
            tell_twin()

    @jax.named_scope("meet_all")
    def meet_all(who):
        @pl.when(who)
        def _():
            pl.semaphore_wait(here, 1)
            tell_twin()

    fine_count = (fine_limit + wide - 1) // wide
    half_way = jnp.minimum(fine_count, 3)
    early = jnp.where(me < 2, 0, jnp.where(me < SUB - 2, 2, jnp.where(me < SUB, 1, 0)))
    early = jnp.minimum(early, half_way)
    many = fine_count > 3
    start(coarse_loads())
    greet()

    @pl.when(many)
    def _():
        start(fine_loads(0))

    start_table()

    @pl.when(jnp.logical_not(many))
    def _():
        start(fine_loads(0))

    start_fine(1)
    picked[...] = jnp.zeros_like(picked)
    picked_m[...] = jnp.zeros_like(picked_m)
    advance_coarse()
    start_fine(2)
    for t in range(mid_tiles):
        start_medium(t)
    for k in range(3, chunks):
        start_fine(k)
    lax.fori_loop(0, early, fine_chunk, 0)
    meet()
    send_first()
    lax.fori_loop(early, half_way, fine_chunk, 0)
    medium_count = (medium_limit + LANES - 1) // LANES
    some = jnp.minimum(medium_count, 1)
    last = a >= quarter + owners
    lax.fori_loop(0, some, medium_chunk, 0)
    hear()
    pairs = (medium_count - some) // 2
    lax.fori_loop(0, pairs, medium_pair, 0)
    lax.fori_loop(some + 2 * pairs, medium_count, medium_chunk, 0)
    meet_all(last)
    lax.fori_loop(half_way, fine_count, fine_chunk, 0)
    put_fine(0, z.groups)
    put_medium()
    meet_all(a < quarter)
    ship()

    @pl.when(owner)
    def _():
        wait_first()
        coarse_rows()

    fill_table(0, n)
    end_table()
    fill_zeros()
    collect()


AHEAD = 2


def ahead_kernel(z, decay_in, amp_in, fine_state, fine_noise, out, state, noise, decay, amp, load, done):
    me = lax.axis_index("scale") * z.lat + lax.axis_index("lat")
    wide = 2 * LANES

    def loads(k):
        cols = pl.ds(k * wide, wide)
        copies = [pltpu.make_async_copy(fine_state.at[:, :, cols], state.at[k], load.at[k])]
        for g in range(z.groups):
            rows = pl.ds(g * SUB, SUB)
            copies.append(pltpu.make_async_copy(fine_noise.at[:, rows, cols], noise.at[k, g], load.at[k]))
        return copies

    def write(k):
        return pltpu.make_async_copy(state.at[k], out.at[:, :, pl.ds(k * wide, wide)], done.at[k])

    @pl.when(me < 2)
    def _():
        scalars = [pltpu.make_async_copy(decay_in, decay, done.at[0]), pltpu.make_async_copy(amp_in, amp, done.at[1])]
        for copy in scalars:
            copy.start()
        for k in range(AHEAD):
            for copy in loads(k):
                copy.start()
        for copy in scalars:
            copy.wait()
        slack = z.fine_slots - me * z.fine - lax.broadcasted_iota(jnp.int32, (SUB, wide), 0)
        slack = slack - lax.broadcasted_iota(jnp.int32, (SUB, wide), 1)
        for k in range(AHEAD):
            for copy in loads(k):
                copy.wait()

            def pair(i, _):
                two = pl.ds(2 * i, 2)
                for g in range(z.groups):
                    rows = slice(g * SUB, (g + 1) * SUB)
                    keep = slack > g * SUB + k * wide
                    new = decay[0] * state[k, two, rows, :] + amp[0] * noise[k, g, two].astype(jnp.float32)
                    state[k, two, rows, :] = jnp.where(keep[None], new, 0.0)
                return 0

            lax.fori_loop(0, z.pairs // 2, pair, 0)
            write(k).start()
        for k in range(AHEAD):
            write(k).wait()


def grid_kernel(
    z, fine_in, medium_in, coarse_in, got, got_coarse, table, begun, fine_out, medium_out, coarse_out, out, turned, sems
):
    me = lax.axis_index("scale") * z.lat + lax.axis_index("lat")
    wide = 2 * LANES

    def ahead():
        cols = pl.ds(0, AHEAD * wide)
        return pltpu.make_async_copy(fine_in.at[:, :, cols], fine_out.at[:, :, cols], sems.at[2 + medium_in.shape[0]])

    @pl.when(me >= 2)
    def _():
        ahead().start()

    rest = pl.ds(AHEAD * wide, z.fine_slots - AHEAD * wide)
    copies = [
        pltpu.make_async_copy(fine_in.at[:, :, rest], fine_out.at[:, :, rest], sems.at[0]),
        pltpu.make_async_copy(coarse_in, coarse_out.at[0], sems.at[1]),
    ]
    for t in range(medium_in.shape[0]):
        cols = pl.ds(t * LANES, LANES)
        copies.append(pltpu.make_async_copy(medium_in.at[t, :, pl.ds(0, z.medium)], medium_out.at[:, :, :, cols], sems.at[2 + t]))
    for copy in copies:
        copy.start()
    with jax.named_scope("turn_rows"):
        turn_rows(z, got, got_coarse, turned)
    with jax.named_scope("sum_longitudes"):
        sum_longitudes(z, turned, table, out)
    with jax.named_scope("wait_writes"):
        for copy in copies:
            copy.wait()

        @pl.when(me >= 2)
        def _():
            ahead().wait()


def turn_rows(z, got, got_coarse, turned):
    many = 2 * z.n * SUB
    turned[:, :many] = got[...].reshape(many, LANES).astype(jnp.float32).T.astype(jnp.bfloat16)
    block = lax.broadcasted_iota(jnp.int32, (SUB, LANES), 1) // z.pairs
    few = []
    for u in range(z.owners // 4):
        for t in range(4):
            rows = jnp.zeros((SUB, LANES), jnp.float32)
            for b in range(4):
                some = got_coarse[4 * u + b].astype(jnp.float32)
                if b != t:
                    some = pltpu.roll(some, (b - t) % 4 * z.pairs, axis=1)
                rows = jnp.where(block == b, some, rows)
            few.append(rows)
    few = jnp.concatenate(few, axis=0)
    turned[:, many:] = few.T.astype(jnp.bfloat16)


def sum_longitudes(z, turned, table, out):
    e, tiles = z.members, z.wrap // LANES
    for t in range(tiles):
        both = jnp.dot(turned[...], table[:, 2 * t * LANES : 2 * (t + 1) * LANES], preferred_element_type=jnp.float32)
        waves = []
        for b in range(4):
            at = 2 * b * e
            cos_r, sin_r = both[at : at + e, :LANES], both[at : at + e, LANES:]
            cos_i, sin_i = both[at + e : at + 2 * e, :LANES], both[at + e : at + 2 * e, LANES:]
            re, im = cos_r - sin_i, sin_r + cos_i
            if b:
                angle = (lax.broadcasted_iota(jnp.int32, (1, LANES), 1) + t * LANES).astype(jnp.float32)
                angle = angle * (2.0 * math.pi * b / NLON)
                cos, sin = jnp.cos(angle), jnp.sin(angle)
                re, im = re * cos - im * sin, re * sin + im * cos
            waves.append((re, im))
        for h in range(4):
            total = None
            for b in range(4):
                re, im = waves[b]
                term = (re, -im, -re, im)[b * h % 4]
                total = term if total is None else total + term
            out[pl.ds(h * tiles + t, e, stride=4 * tiles), :] = jnp.tanh(total)


def fast_body(
    z,
    fine_state,
    fine_noise,
    medium_state,
    medium_noise,
    coarse_state,
    coarse_noise,
    decay,
    amplitude,
    fine_basis,
    medium_basis,
    coarse_basis,
):
    f32, bf16, dma = jnp.float32, jnp.bfloat16, pltpu.SemaphoreType.DMA
    e, n, lat, rows = z.members, z.n, z.lat, z.rows
    tiles = z.medium_slots // LANES
    owners = z.owners
    table_rows = 2 * n * SUB + owners * SUB
    operands = (
        decay,
        amplitude,
        fine_state.reshape(z.pairs, z.fine, z.fine_slots),
        fine_noise.reshape(z.pairs, z.fine, z.fine_slots),
        fine_basis,
        medium_state.transpose(0, 2, 1, 3),
        medium_noise.transpose(0, 2, 1, 3),
        medium_basis,
        coarse_state,
        coarse_noise,
        coarse_basis,
    )
    operands = tuple(pltpu.with_memory_space_constraint(x, pltpu.HBM) for x in operands)
    vmem = pl.BlockSpec(memory_space=pltpu.VMEM)
    hbm = pl.BlockSpec(memory_space=pltpu.HBM)
    between = (
        pltpu.VMEM((z.pairs, z.fine, z.fine_slots), f32),
        pltpu.VMEM((tiles, e, z.medium_room, 2, LANES), f32),
        pltpu.VMEM((2, z.coarse, z.coarse_slots), f32),
        pltpu.VMEM((n, 2 * SUB, LANES), bf16),
        pltpu.VMEM((owners, SUB, LANES), bf16),
        pltpu.VMEM((table_rows, 2 * z.wrap), bf16),
    )
    begun = pl.pallas_call(
        functools.partial(ahead_kernel, z),
        out_shape=jax.ShapeDtypeStruct((z.pairs, z.fine, z.fine_slots), f32),
        in_specs=[hbm] * 4,
        out_specs=hbm,
        scratch_shapes=[
            pltpu.VMEM((AHEAD, z.pairs, z.fine, 2 * LANES), f32),
            pltpu.VMEM((AHEAD, z.groups, z.pairs, SUB, 2 * LANES), bf16),
            pltpu.SMEM((3,), f32),
            pltpu.SMEM((3,), f32),
            dma((AHEAD,)),
            dma((AHEAD,)),
        ],
        compiler_params=pltpu.CompilerParams(vmem_limit_bytes=32 * 1024 * 1024),
    )(*operands[:4])
    begun = pltpu.with_memory_space_constraint(begun, pltpu.HBM)
    held = pl.pallas_call(
        functools.partial(spread_kernel, z),
        out_shape=between,
        in_specs=[hbm] * 12,
        out_specs=(vmem,) * 6,
        scratch_shapes=[
            pltpu.VMEM((z.groups, z.pairs, SUB, z.fine_slots), bf16),
            pltpu.VMEM((z.fine, rows, z.fine_slots), bf16),
            pltpu.VMEM((z.groups, SUB * z.pairs, 2 * LANES), bf16),
            pltpu.VMEM((z.groups * rows, 2 * LANES), f32),
            pltpu.VMEM((tiles, e, z.medium, 2, LANES), bf16),
            pltpu.VMEM((tiles, z.medium, rows, LANES), bf16),
            pltpu.VMEM((2, z.medium * z.pairs, LANES), bf16),
            pltpu.VMEM((z.medium // 4 * rows, LANES), f32),
            pltpu.VMEM((rows * 3 * SUB, LANES), f32),
            pltpu.VMEM((n, 2 * SUB, LANES), bf16),
            pltpu.VMEM((2, z.coarse, z.coarse_slots), bf16),
            pltpu.VMEM((z.coarse, z.coarse_slots), bf16),
            pltpu.VMEM((max(z.first_rows * owners, lat * 3 * SUB), LANES), f32),
            pltpu.VMEM((owners, z.first_rows, LANES), bf16),
            pltpu.VMEM((lat, z.first_rows, LANES), bf16),
            pltpu.VMEM((lat * (z.first_rows + SUB), LANES), f32),
            pltpu.VMEM(((2 * z.piece - z.low) * lat, LANES), bf16),
            pltpu.VMEM((z.low * z.pairs, LANES), bf16),
            pltpu.VMEM((lat, SUB, LANES), bf16),
            pltpu.VMEM((2 * n, z.wrap), f32),
            pltpu.VMEM((2 * n, z.wrap), f32),
            pltpu.SMEM((3,), f32),
            pltpu.SMEM((3,), f32),
            dma((z.fine_slots // (2 * LANES),)),
            dma((tiles,)),
            dma,
            dma((3,)),
            dma((3,)),
            pltpu.SemaphoreType.REGULAR,
            pltpu.SemaphoreType.REGULAR,
        ],
        compiler_params=pltpu.CompilerParams(
            collective_id=0, has_side_effects=True, vmem_limit_bytes=32 * 1024 * 1024
        ),
    )(*operands, begun)
    fine_next, medium_next, coarse_next, pattern = pl.pallas_call(
        functools.partial(grid_kernel, z),
        out_shape=(
            jax.ShapeDtypeStruct((z.pairs, z.fine, z.fine_slots), f32),
            jax.ShapeDtypeStruct((e, z.medium, 2, z.medium_slots), f32),
            jax.ShapeDtypeStruct(coarse_state.shape, f32),
            jax.ShapeDtypeStruct((e * NLON // LANES, LANES), f32),
        ),
        in_specs=[vmem] * 6 + [hbm],
        out_specs=(hbm, hbm, hbm, vmem),
        input_output_aliases={6: 0},
        scratch_shapes=[pltpu.VMEM((LANES, table_rows), bf16), dma((3 + tiles,))],
        compiler_params=pltpu.CompilerParams(vmem_limit_bytes=32 * 1024 * 1024),
    )(*held, begun)
    return (
        fine_next.reshape(fine_state.shape),
        medium_next.transpose(0, 2, 1, 3),
        coarse_next,
        pattern.reshape(e, 1, NLON),
    )


def body(*arrays):
    fine_state, medium_state, coarse_state = arrays[0], arrays[2], arrays[4]
    scale, lat = lax.axis_size("scale"), lax.axis_size("lat")
    z = Sizes(fine_state, medium_state, coarse_state, arrays[8], arrays[10], scale, lat)
    return fast_body(z, *arrays) if z.fits() else general_body(*arrays)


def solution(mesh):
    return jax.shard_map(
        body,
        mesh=mesh,
        in_specs=(
            P(None, None, ("scale", "lat"), None),
            P(None, None, ("scale", "lat"), None),
            P(None, None, ("scale", "lat"), None),
            P(None, None, ("scale", "lat"), None),
            P("lat", None, None, None),
            P("lat", None, None, None),
            P(),
            P(),
            P(("scale", "lat"), None, None),
            P(("scale", "lat"), None, None),
            P(("scale", "lat"), None, None),
        ),
        out_specs=(
            P(None, None, ("scale", "lat"), None),
            P(None, None, ("scale", "lat"), None),
            P("lat", None, None, None),
            P(None, ("scale", "lat"), None),
        ),
        check_vma=False,
    )
```
